128 devices in a mesh: leaf: 32 (over x, z, core), band: 4 (over y).
Axes of the slice: x: 4, y: 4, z: 4, core: 2. Of those that a mesh axis runs over, the one named last changes fastest.
Arguments:
- excitation: float32 [16, 8, 65536], P(None, None, 'leaf'), may hold values from -6 to 6
- freq_index: int32 [4], P('band'), may hold values from 1 to 3
- elem_order: int32 [32, 2048], P('leaf'), may hold values from 0 to 2047, each once within a row
- level_factors: bfloat16 [4, 32, 9, 2, 2, 128, 128], P('band', 'leaf'), may hold values from -1 to 1
- image_weights: bfloat16 [4, 2, 16, 65536], P('band', None, None, 'leaf'), may hold values from -1 to 1
- coupling: bfloat16 [4, 2, 128, 128], P('band'), may hold values from -0.375 to 0.375
- reflectivity: bfloat16 [65536, 128], P('leaf'), may hold values from -4 to 4
- clip_level: int32 [16], replicated, may hold values from 0 to 8
Outputs:
- retransmit: float32 [16, 8, 65536], P(None, None, 'leaf')
The draws below stay inside these ranges and needn't reach their ends.
Inputs may be any that keep to these rules, and one draw needn't show every extreme that they name: `elem_order`: each row holds every number from 0 to 2047 once.
All inputs are finite; a program needn't handle non-finite values.
Results may differ from the reference program's by a relative error of at most 0.014.
Values sent between devices are 32-bit elements; how exact they have to be, the bound alone decides.
No kernel may reach another device: no remote copies, remote signals or barrier semaphores. Data moves between devices by JAX's collectives and lax.ppermute only.
A program may use at most 64 MiB of HBM per device.

```python
import math
import jax
import jax.numpy as jnp
from jax import lax

ELEMENTS = 65536
IMAGE = 8388608
RANK = 128
LEVELS = 9
SAMPLES = 8
ITERS = 2
SHOTS = 16
BANDS = 4
E_DEV = 2048
BOXES = 16
IMG_DEV = 2048
N_LEAF = 32


def draw_level_factors(key, part):
    shape = (BANDS, N_LEAF, LEVELS, 2, 2, RANK, RANK)
    base = jax.random.normal(key, shape, jnp.float32) * (4.0 * RANK) ** (-0.5)
    base = jnp.clip(base, -6.0 * (4.0 * RANK) ** (-0.5), 6.0 * (4.0 * RANK) ** (-0.5))
    rise = jnp.log(3.0)
    leaf_pos = jnp.arange(N_LEAF, dtype=jnp.float32) / (N_LEAF - 1)
    leaf_scale = jnp.exp(rise * leaf_pos) / jnp.exp(rise * 0.5)
    level_pick = (jnp.arange(LEVELS) == 0).astype(jnp.float32)
    factor = 1.0 + (leaf_scale[:, None] - 1.0) * level_pick[None, :]
    scaled = base * factor[None, :, :, None, None, None, None]
    scaled = jnp.clip(scaled, -0.99, 0.99)
    return scaled.astype(jnp.bfloat16)


def plant(array, rng, low, largest):
    longest = array.shape.index(max(array.shape))
    spots = []
    for shift in (0, 1):
        where = [jax.random.randint(jax.random.fold_in(rng, axis), (), 0, length) for axis, length in enumerate(array.shape)]
        where[longest] = (where[longest] + shift) % array.shape[longest]
        spots.append(tuple(where))
    return array.at[spots[0]].set(low).at[spots[1]].set(largest)


def shard_levels(rng, dims, split, smallest, largest):
    level = 1.0
    for axis_at, blocks in split:
        heights = jax.random.uniform(jax.random.fold_in(jax.random.fold_in(rng, 6), axis_at), (blocks,), jnp.float32, smallest / len(split), largest / len(split))
        level = level * jnp.repeat(jnp.exp(heights), dims[axis_at] // blocks).reshape((-1,) + (1,) * (len(dims) - 1 - axis_at))
    return level


def scatter_about(key, extent, width, limit, shards=(), kind=jnp.bfloat16):
    values = jax.random.normal(key, extent, jnp.float32) * width
    if len(shards) > 0:
        values = shard_levels(key, extent, shards, -0.22, 0.18) * values
    return jnp.clip(values, min=-limit, max=limit).astype(kind)


def setup_inputs(seed: int = 0) -> dict:
    key_list = jax.random.split(jax.random.key(seed), 9)
    return {
        "excitation": scatter_about(key_list[0], (SHOTS, SAMPLES, ELEMENTS), 1.0, 6.0, ((2, 32),), jnp.float32),
        "freq_index": plant(jax.random.randint(key_list[1], (BANDS,), 1, SAMPLES // 2), jax.random.fold_in(key_list[1], 1), 1, (SAMPLES // 2) - 1).astype(jnp.int32),
        "elem_order": jax.vmap(lambda own: jax.random.permutation(own, E_DEV))(jax.random.split(key_list[2], N_LEAF)).reshape((N_LEAF, E_DEV)).astype(jnp.int32),
        "level_factors": draw_level_factors(jax.random.fold_in(key_list[8], 71), 0),
        "image_weights": scatter_about(key_list[4], (BANDS, 2, BOXES, IMAGE // RANK), (2 * BOXES) ** -0.5, 1.0, ((0, 4), (3, 32))),
        "coupling": scatter_about(key_list[5], (BANDS, 2, RANK, RANK), (2 * RANK) ** -0.5, 0.375, ((0, 4),)),
        "reflectivity": scatter_about(key_list[6], (IMAGE // RANK, RANK), 1.0, 4.0, ((0, 32),)),
        "clip_level": plant(jax.random.randint(key_list[7], (SHOTS,), 0, 9), jax.random.fold_in(key_list[7], 1), 0, 8).astype(jnp.int32),
    }


def block_form(real_part, imag_part):
    top_rows = jnp.concatenate([real_part, imag_part], axis=-1)
    bottom_rows = jnp.concatenate([-imag_part, real_part], axis=-1)
    return jnp.concatenate([top_rows, bottom_rows], axis=-2)

def flip_pairs(values, axis_num, bit_num):
    moved = jnp.moveaxis(values, axis_num, 0)
    lead_count = moved.shape[0]
    half_span = 1 << bit_num
    folded = moved.reshape((lead_count // (2 * half_span), 2, half_span) + moved.shape[1:])
    folded = folded[:, ::-1]
    return jnp.moveaxis(folded.reshape(moved.shape), 0, axis_num)

def image_pass(coeffs, weights, reflect, couple_mat):
    turned = jnp.concatenate([-coeffs[..., RANK:], coeffs[..., :RANK]], axis=-1)
    stacked = jnp.concatenate([coeffs, turned], axis=0).reshape(2 * BOXES, SHOTS * 2 * RANK)
    flat_weights = weights.reshape(2 * BOXES, IMG_DEV)
    image_field = lax.dot_general(flat_weights, stacked, (((0,), (0,)), ((), ())), preferred_element_type=jnp.float32)
    image_field = image_field.reshape(IMG_DEV, SHOTS, 2 * RANK)
    reflect_pair = jnp.concatenate([reflect, reflect], axis=-1).astype(jnp.float32)[:, None, :]
    scaled = (reflect_pair * image_field).astype(jnp.bfloat16)
    coupled = jnp.dot(scaled.reshape(IMG_DEV * SHOTS, 2 * RANK), couple_mat, preferred_element_type=jnp.float32)
    coupled = coupled.reshape(IMG_DEV, SHOTS, 2 * RANK)
    echo_field = (reflect_pair * (image_field + coupled)).astype(jnp.bfloat16)
    turned_back = jnp.concatenate([echo_field[..., RANK:], -echo_field[..., :RANK]], axis=-1)
    summed = jnp.dot(weights[0], echo_field.reshape(IMG_DEV, SHOTS * 2 * RANK), preferred_element_type=jnp.float32)
    summed = summed + jnp.dot(weights[1], turned_back.reshape(IMG_DEV, SHOTS * 2 * RANK), preferred_element_type=jnp.float32)
    return summed.reshape(BOXES, SHOTS, 2 * RANK)

def reference(excitation, freq_index, elem_order, level_factors, image_weights, coupling, reflectivity, clip_level):
    highest = lax.Precision.HIGHEST
    local_levels = BOXES.bit_length() - 1
    self_mats = block_form(level_factors[:, :, :, 0, 0], level_factors[:, :, :, 0, 1])
    cross_mats = block_form(level_factors[:, :, :, 1, 0], level_factors[:, :, :, 1, 1])
    global_perm = (jnp.arange(N_LEAF, dtype=jnp.int32)[:, None] * E_DEV + elem_order).reshape(-1).astype(jnp.int32)
    inverse = jnp.argsort(global_perm).astype(jnp.int32)
    reflect_leaf = reflectivity.reshape(N_LEAF, IMG_DEV, RANK)
    time_steps = jnp.arange(SAMPLES, dtype=jnp.float32)
    clip_scale = (4.0 + clip_level.astype(jnp.float32)) / 10.0
    signal = excitation
    for iteration in range(ITERS):
        summed = jnp.zeros((SHOTS, SAMPLES, ELEMENTS), jnp.float32)
        for band_idx in range(BANDS):
            phase_angle = 2.0 * math.pi / SAMPLES * freq_index[band_idx].astype(jnp.float32) * time_steps
            cosine = jnp.cos(phase_angle)
            sine_table = jnp.sin(phase_angle)
            spec_real = lax.optimization_barrier(jnp.sum(signal * cosine[None, :, None], axis=1))[:, global_perm]
            spec_imag = (-lax.optimization_barrier(jnp.sum(signal * sine_table[None, :, None], axis=1)))[:, global_perm]
            joined = jnp.concatenate([spec_real.reshape(SHOTS, N_LEAF, BOXES, RANK), spec_imag.reshape(SHOTS, N_LEAF, BOXES, RANK)], axis=-1)
            coeffs = joined.transpose(1, 2, 0, 3).astype(jnp.float32)
            band_self = self_mats[band_idx].astype(jnp.float32)
            band_cross = cross_mats[band_idx].astype(jnp.float32)
            for level_idx in range(LEVELS):
                if level_idx < local_levels:
                    partner = flip_pairs(coeffs, 1, level_idx)
                else:
                    partner = flip_pairs(coeffs, 0, level_idx - local_levels)
                coeffs = jnp.einsum('lbsk,lkm->lbsm', coeffs, band_self[:, level_idx], precision=highest) + jnp.einsum('lbsk,lkm->lbsm', partner, band_cross[:, level_idx], precision=highest)
            weights_leaf = image_weights[band_idx].reshape(2, BOXES, N_LEAF, IMG_DEV).transpose(2, 0, 1, 3)
            couple_mat = block_form(coupling[band_idx, 0], coupling[band_idx, 1])
            coeffs = lax.map(lambda items: image_pass(items[0], items[1], items[2], couple_mat), (coeffs.astype(jnp.bfloat16), weights_leaf, reflect_leaf))
            for level_idx in reversed(range(LEVELS)):
                outgoing = jnp.einsum('lbsm,lkm->lbsk', coeffs, band_cross[:, level_idx], precision=highest)
                if level_idx < local_levels:
                    incoming = flip_pairs(outgoing, 1, level_idx)
                else:
                    incoming = flip_pairs(outgoing, 0, level_idx - local_levels)
                coeffs = jnp.einsum('lbsm,lkm->lbsk', coeffs, band_self[:, level_idx], precision=highest) + incoming
            real_part = coeffs[..., :RANK].transpose(2, 0, 1, 3).reshape(SHOTS, ELEMENTS)[:, inverse]
            imag_part = coeffs[..., RANK:].transpose(2, 0, 1, 3).reshape(SHOTS, ELEMENTS)[:, inverse]
            summed = summed + real_part[:, None, :] * cosine[None, :, None] - imag_part[:, None, :] * sine_table[None, :, None]
        energy = lax.optimization_barrier(jnp.sum(summed * summed, axis=(1, 2)))
        root_mean = jnp.sqrt(energy / (SAMPLES * ELEMENTS) + 1e-06)
        clip_amp = (clip_scale * root_mean)[:, None, None]
        signal = jnp.clip(summed, -clip_amp, clip_amp) / clip_amp
    return signal
```

```python
import functools
import math

import jax
import jax.numpy as jnp
from jax import lax
from jax.experimental import pallas as pl
from jax.experimental.pallas import tpu as pltpu
from jax.sharding import Mesh
from jax.sharding import PartitionSpec as P

ELEMENTS = 65536
ITERS = 2
RANK = 128
BOXES = 16
LOCAL_LEVELS = 4
SAMPLES = 8
Q_BLOCK = 256
LEAF = ("leaf_0", "leaf_1", "leaf_2")
F32 = jnp.float32
BF16 = jnp.bfloat16
VMEM = pl.BlockSpec(memory_space=pltpu.VMEM)
SMEM = pl.BlockSpec(memory_space=pltpu.SMEM)


def dot(left, right):
    return jnp.dot(left, right, preferred_element_type=F32)


def dot_t(left, right):
    return lax.dot_general(left, right, (((1,), (1,)), ((), ())), preferred_element_type=F32)


def block_form(real_part, imag_part):
    top_rows = jnp.concatenate([real_part, imag_part], axis=1)
    bottom_rows = jnp.concatenate([-imag_part, real_part], axis=1)
    return jnp.concatenate([top_rows, bottom_rows], axis=0)


def factor(ref, level, side):
    return block_form(ref[level, side, 0], ref[level, side, 1])


def far_factor(ref, side):
    return block_form(ref[side, 0], ref[side, 1]).astype(BF16)


def split(value):
    high = value.astype(BF16)
    low = (value - high.astype(F32)).astype(BF16)
    return jnp.concatenate([high, low], axis=0)


def joined(product):
    rows = product.shape[0] // 2
    return product[:rows] + product[rows:]


def paired(ref):
    return jnp.concatenate([ref[0], ref[1]], axis=1)


def put(ref, value):
    ref[0] = value[:, :RANK]
    ref[1] = value[:, RANK:]


def flip_boxes(value, level):
    span = value.shape[0] // BOXES << level
    parts = [value[at : at + span] for at in range(0, value.shape[0], span)]
    return jnp.concatenate([parts[at ^ 1] for at in range(len(parts))], axis=0)


def cosine(step):
    half = math.sqrt(0.5)
    diagonal = jnp.where((step == 1) | (step == 7), F32(half), F32(-half))
    straight = jnp.where(step == 0, F32(1.0), jnp.where(step == 4, F32(-1.0), F32(0.0)))
    return jnp.where((step & 1) == 1, diagonal, straight)


def wave(freq):
    cos_values = [cosine((freq * time) & 7) for time in range(SAMPLES)]
    sin_values = [cosine((freq * time + 6) & 7) for time in range(SAMPLES)]
    return cos_values, sin_values


def local_forward(coeffs, factors):
    for level in range(LOCAL_LEVELS):
        parts = split(coeffs)
        own = joined(dot(parts, factor(factors, level, 0)))
        cross = joined(dot(parts, factor(factors, level, 1)))
        coeffs = own + flip_boxes(cross, level)
    return coeffs


def first_kernel(signal, freq, order, factors, out, spectrum):
    shots = signal.shape[0]
    cos_values, sin_values = wave(freq[0])
    rows = lax.broadcasted_iota(jnp.int32, (SAMPLES, 1), 0)
    cos_column = jnp.zeros((SAMPLES, 1), F32)
    sin_column = jnp.zeros((SAMPLES, 1), F32)
    for time in range(SAMPLES):
        cos_column = jnp.where(rows == time, cos_values[time], cos_column)
        sin_column = jnp.where(rows == time, -sin_values[time], sin_column)
    for shot in range(shots):
        value = signal[shot]
        spectrum[shot : shot + 1, :] = jnp.sum(value * cos_column, axis=0, keepdims=True)
        spectrum[shots + shot : shots + shot + 1, :] = jnp.sum(
            value * sin_column, axis=0, keepdims=True
        )
    parts = split(spectrum[...])
    elements = parts.shape[1]
    element = lax.broadcasted_iota(jnp.int32, (elements, 2 * RANK), 0)
    real_rows = []
    imag_rows = []
    for pair in range(BOXES // 2):
        place = order[:, pair * 2 * RANK : (pair + 1) * 2 * RANK]
        chosen = jnp.where(element == place, F32(1.0), F32(0.0)).astype(BF16)
        placed = joined(dot(parts, chosen))
        for half in range(2):
            lanes = slice(half * RANK, (half + 1) * RANK)
            real_rows.append(placed[:shots, lanes])
            imag_rows.append(placed[shots:, lanes])
    coeffs = jnp.concatenate(
        [jnp.concatenate(real_rows, axis=0), jnp.concatenate(imag_rows, axis=0)], axis=1
    )
    put(out, local_forward(coeffs, factors))


def core_kernel(own, other, factors, out):
    level = LOCAL_LEVELS
    put(
        out,
        joined(dot(split(paired(own)), factor(factors, level, 0)))
        + joined(dot(split(paired(other)), factor(factors, level, 1))),
    )


def two_levels(own, near, far, both, factors, far_factors, level):
    first = joined(dot(split(paired(own)), factor(factors, level, 0))) + joined(
        dot(split(paired(near)), factor(factors, level, 1))
    )
    second = joined(dot(split(paired(far)), far_factor(far_factors, 0))) + joined(
        dot(split(paired(both)), far_factor(far_factors, 1))
    )
    return joined(dot(split(first), factor(factors, level + 1, 0))) + joined(
        dot(split(second), factor(factors, level + 1, 1))
    )


def two_adjoints(coeffs, factors, far_factors, level, own, near, far, both):
    parts = split(coeffs)
    first = split(joined(dot_t(parts, factor(factors, level + 1, 0))))
    second = split(joined(dot_t(parts, factor(factors, level + 1, 1))))
    put(own, joined(dot_t(first, factor(factors, level, 0))))
    put(near, joined(dot_t(first, factor(factors, level, 1))))
    put(far, joined(dot_t(second, far_factor(far_factors, 0))))
    put(both, joined(dot_t(second, far_factor(far_factors, 1))))


def forward_kernel(own, near, far, both, factors, far_factors, out, *, level):
    put(out, two_levels(own, near, far, both, factors, far_factors, level))


def adjoint_kernel(a, b, c, d, factors, far_factors, own, near, far, both, *, level):
    coeffs = (paired(a) + paired(b)) + (paired(c) + paired(d))
    two_adjoints(coeffs, factors, far_factors, level, own, near, far, both)


def core_adjoint_kernel(a, b, c, d, factors, own, other):
    level = LOCAL_LEVELS
    parts = split((paired(a) + paired(b)) + (paired(c) + paired(d)))
    put(own, joined(dot_t(parts, factor(factors, level, 0))))
    put(other, joined(dot_t(parts, factor(factors, level, 1))))


def local_adjoint_kernel(own, other, factors, out):
    coeffs = paired(own) + paired(other)
    for level in reversed(range(LOCAL_LEVELS)):
        parts = split(coeffs)
        cross = joined(dot_t(parts, factor(factors, level, 1)))
        coeffs = joined(dot_t(parts, factor(factors, level, 0))) + flip_boxes(cross, level)
    put(out, coeffs)


def image_kernel(
    own0, near0, far0, both0, factors, far_factors, weights, reflect, coupling,
    own, near, far, both,
    coeffs, stacked, scaled, field, total,
    *, level, shots,
):
    entered = two_levels(own0, near0, far0, both0, factors, far_factors, level)
    put(coeffs, entered)
    lanes = 2 * RANK
    for shot in range(shots):
        real = coeffs[0, pl.ds(shot, BOXES, stride=shots), :]
        imag = coeffs[1, pl.ds(shot, BOXES, stride=shots), :]
        rows = jnp.concatenate([real, imag], axis=1)
        turned = jnp.concatenate([-imag, real], axis=1)
        stacked[:, shot * lanes : (shot + 1) * lanes] = jnp.concatenate(
            [rows, turned], axis=0
        ).astype(BF16)
    total[...] = jnp.zeros_like(total)
    couple = block_form(coupling[0], coupling[1])
    block = Q_BLOCK

    @pl.loop(0, weights.shape[1] // block)
    def _(turn):
        start = pl.multiple_of(turn * block, block)
        weight = weights[:, pl.ds(start, block)]
        weight_t = weight.astype(F32).T.astype(BF16)
        rho = reflect[pl.ds(start, block), :].astype(F32)
        rho = jnp.concatenate([rho, rho], axis=1)
        for shot in range(shots):
            at = slice(shot * block, (shot + 1) * block)
            value = dot(weight_t, stacked[:, shot * lanes : (shot + 1) * lanes])
            field[at, :] = value
            scaled[at, :] = (rho * value).astype(BF16)
        coupled = dot(scaled[...], couple)
        for shot in range(shots):
            at = slice(shot * block, (shot + 1) * block)
            echo = (rho * (field[at, :] + coupled[at])).astype(BF16)
            total[:, shot * lanes : (shot + 1) * lanes] += dot(weight, echo)

    for shot in range(shots):
        real = total[:BOXES, shot * lanes : (shot + 1) * lanes]
        imag = total[BOXES:, shot * lanes : (shot + 1) * lanes]
        coeffs[0, pl.ds(shot, BOXES, stride=shots), :] = real[:, :RANK] + imag[:, RANK:]
        coeffs[1, pl.ds(shot, BOXES, stride=shots), :] = real[:, RANK:] - imag[:, :RANK]
    two_adjoints(paired(coeffs), factors, far_factors, level, own, near, far, both)


def summed_kernel(s0, s1, s2, s3, f0, f1, f2, f3, out, energy, *, shots, last):
    waves = [wave(freq[0]) for freq in (f0, f1, f2, f3)]
    spectra = (s0, s1, s2, s3)
    power = jnp.zeros((shots, RANK), F32)
    for box in range(BOXES):
        rows = slice(box * shots, (box + 1) * shots)
        for time in range(SAMPLES):
            value = jnp.zeros((shots, RANK), F32)
            for (cos_values, sin_values), spectrum in zip(waves, spectra):
                value = value + spectrum[0, rows, :] * cos_values[time]
                value = value - spectrum[1, rows, :] * sin_values[time]
            power = power + value * value
            if last:
                out[box, pl.ds(time, shots, stride=SAMPLES), :] = value
            else:
                out[time, rows, :] = value
    column = jnp.sum(power, axis=1, keepdims=True)
    at_shot = lax.broadcasted_iota(jnp.int32, (shots, RANK), 0)
    at_lane = lax.broadcasted_iota(jnp.int32, (shots, RANK), 1)
    row = jnp.sum(jnp.where(at_shot == at_lane, column, F32(0.0)), axis=0, keepdims=True)
    energy[...] = jnp.broadcast_to(row, energy.shape)


def amplitude(energy, clip_level, shots):
    row = jnp.sum(energy[...], axis=0, keepdims=True)
    root_mean = jnp.sqrt(row / (SAMPLES * ELEMENTS) + 1e-6)[:, :shots]
    row = (4.0 + clip_level[...].astype(F32)) / 10.0 * root_mean
    at_shot = lax.broadcasted_iota(jnp.int32, (shots, shots), 0)
    at_lane = lax.broadcasted_iota(jnp.int32, (shots, shots), 1)
    return jnp.sum(jnp.where(at_shot == at_lane, row, F32(0.0)), axis=1, keepdims=True)


def next_kernel(summed, energy, clip_level, freq, factors, out, *, shots):
    amp = jnp.broadcast_to(amplitude(energy, clip_level, shots), (shots, RANK))
    inverse = 1.0 / amp
    cos_values, sin_values = wave(freq[0])
    real_rows = []
    imag_rows = []
    for box in range(BOXES):
        rows = slice(box * shots, (box + 1) * shots)
        real = jnp.zeros((shots, RANK), F32)
        imag = jnp.zeros((shots, RANK), F32)
        for time in range(SAMPLES):
            value = jnp.clip(summed[time, rows, :], -amp, amp)
            real = real + value * cos_values[time]
            imag = imag - value * sin_values[time]
        real_rows.append(real * inverse)
        imag_rows.append(imag * inverse)
    coeffs = jnp.concatenate(
        [jnp.concatenate(real_rows, axis=0), jnp.concatenate(imag_rows, axis=0)], axis=1
    )
    put(out, local_forward(coeffs, factors))


def order_kernel(summed, order, out):
    left = jnp.concatenate([summed[box] for box in range(BOXES)], axis=1)
    parts = split(left)
    elements = parts.shape[1]
    element = lax.broadcasted_iota(jnp.int32, (2 * RANK, elements), 0)
    for tile in range(elements // (2 * RANK)):
        chosen = jnp.where(order[...] == element + tile * 2 * RANK, F32(1.0), F32(0.0))
        placed = joined(dot_t(parts, chosen.astype(BF16)))
        out[:, tile * 2 * RANK : (tile + 1) * 2 * RANK] = placed


def clip_kernel(summed, energy, clip_level, out, *, shots):
    amp = amplitude(energy, clip_level, shots)
    for shot in range(shots):
        limit = jnp.broadcast_to(amp[shot : shot + 1, :], (SAMPLES, 1))
        value = summed[shot * SAMPLES : (shot + 1) * SAMPLES, :]
        out[shot] = jnp.clip(value, -limit, limit) / limit


def call(body, outs, operands, smem=(), scratch=(), limit=24, flops=0, name=None, **settings):
    return pl.pallas_call(
        functools.partial(body, **settings) if settings else body,
        out_shape=outs,
        in_specs=[SMEM if at in smem else VMEM for at in range(len(operands))],
        out_specs=jax.tree.map(lambda _: VMEM, outs),
        scratch_shapes=list(scratch),
        compiler_params=pltpu.CompilerParams(vmem_limit_bytes=limit << 20),
        cost_estimate=pl.CostEstimate(flops=flops, transcendentals=0, bytes_accessed=1 << 20),
        name=name,
    )(*operands)


def exchange(values, axis):
    received = []
    for step, value in enumerate(values, 1):
        pairs = [(source, source ^ step) for source in range(lax.axis_size(axis))]
        received.append(lax.ppermute(value, axis, pairs))
    return received


def on_device(
    excitation,
    freq_index,
    elem_order,
    level_factors,
    image_weights,
    coupling,
    reflectivity,
    clip_level,
):
    shots = excitation.shape[0]
    rows = shots * BOXES
    leaves = lax.axis_size(LEAF)
    factors = level_factors[0, 0]
    weights = image_weights[0].reshape(2 * BOXES, image_weights.shape[3])
    couple = coupling[0]
    clips = clip_level.reshape(1, shots)
    coeff = jax.ShapeDtypeStruct((2, rows, RANK), F32)
    freqs = [freq_index] + exchange([freq_index] * 3, "band")

    def far_level(level, axis):
        pairs = [(source, source ^ 2) for source in range(lax.axis_size(axis))]
        return lax.ppermute(factors[level].astype(F32), axis, pairs)

    far_z = far_level(5, "leaf_1")
    far_x = far_level(7, "leaf_0")
    coeffs = call(
        first_kernel,
        coeff,
        (excitation, freq_index, elem_order, factors),
        smem=(1,),
        scratch=[pltpu.VMEM((2 * shots, excitation.shape[2]), F32)],
        flops=8_000_000_000,
        name="first",
    )
    for iteration in range(ITERS):
        last = iteration == ITERS - 1
        (other,) = exchange([coeffs], "leaf_2")
        coeffs = call(
            core_kernel, coeff, (coeffs, other, factors), flops=1_000_000_000, name="core"
        )
        received = exchange([coeffs] * 3, "leaf_1")
        coeffs = call(
            forward_kernel,
            coeff,
            (coeffs, *received, factors, far_z),
            flops=2_000_000_000,
            name="forward",
            level=5,
        )
        received = exchange([coeffs] * 3, "leaf_0")
        own, *sent = call(
            image_kernel,
            (coeff,) * 4,
            (coeffs, *received, factors, far_x, weights, reflectivity, couple),
            scratch=[
                pltpu.VMEM((2, rows, RANK), F32),
                pltpu.VMEM((2 * BOXES, shots * 2 * RANK), BF16),
                pltpu.VMEM((shots * Q_BLOCK, 2 * RANK), BF16),
                pltpu.VMEM((shots * Q_BLOCK, 2 * RANK), F32),
                pltpu.VMEM((2 * BOXES, shots * 2 * RANK), F32),
            ],
            limit=40,
            flops=15_000_000_000,
            name="image",
            level=7,
            shots=shots,
        )
        own, *sent = call(
            adjoint_kernel,
            (coeff,) * 4,
            (own, *exchange(sent, "leaf_0"), factors, far_z),
            flops=2_000_000_000,
            name="adjoint",
            level=5,
        )
        own, sent = call(
            core_adjoint_kernel,
            (coeff,) * 2,
            (own, *exchange(sent, "leaf_1"), factors),
            flops=1_000_000_000,
            name="core_adjoint",
        )
        (other,) = exchange([sent], "leaf_2")
        spectrum = call(
            local_adjoint_kernel,
            coeff,
            (own, other, factors),
            flops=2_000_000_000,
            name="local_adjoint",
        )
        received = exchange([spectrum] * 3, "band")
        shape = (BOXES, shots * SAMPLES, RANK) if last else (SAMPLES, rows, RANK)
        summed, energy = call(
            summed_kernel,
            (jax.ShapeDtypeStruct(shape, F32), jax.ShapeDtypeStruct((leaves, RANK), F32)),
            (spectrum, *received, *freqs),
            smem=(4, 5, 6, 7),
            flops=1_000_000_000,
            name="summed",
            shots=shots,
            last=last,
        )
        energy = lax.all_to_all(energy, LEAF, 0, 0, tiled=True)
        if last:
            ordered = call(
                order_kernel,
                jax.ShapeDtypeStruct((shots * SAMPLES, excitation.shape[2]), F32),
                (summed, elem_order),
                flops=3_000_000_000,
                name="order",
            )
            return call(
                clip_kernel,
                jax.ShapeDtypeStruct(excitation.shape, F32),
                (ordered, energy, clips),
                flops=500_000_000,
                name="clip",
                shots=shots,
            )
        coeffs = call(
            next_kernel,
            coeff,
            (summed, energy, clips, freq_index, factors),
            smem=(3,),
            flops=2_000_000_000,
            name="next",
            shots=shots,
        )


def solution(mesh):
    finer = Mesh(
        mesh.devices.reshape(4, 4, 2, mesh.shape["band"]), ("leaf_0", "leaf_1", "leaf_2", "band")
    )
    placed = (
        P(None, None, LEAF),
        P("band"),
        P(LEAF, None),
        P("band", LEAF, None, None, None, None, None),
        P("band", None, None, LEAF),
        P("band", None, None, None),
        P(LEAF, None),
        P(),
    )
    return jax.shard_map(
        on_device, mesh=finer, in_specs=placed, out_specs=P(None, None, LEAF), check_vma=False
    )
```

```python
import math

import jax
import jax.numpy as jnp
from jax import lax
from jax.experimental import pallas as pl
from jax.experimental.pallas import tpu as pltpu
from jax.sharding import Mesh
from jax.sharding import PartitionSpec as P

ELEMENTS = 65536
ITERS = 2
RANK = 128
BOXES = 16
LOCAL_LEVELS = 4
SAMPLES = 8
Q_BLOCK = 512
GROUPS = 2
LEAF = ("leaf_0", "leaf_1", "leaf_2")
F32 = jnp.float32
BF16 = jnp.bfloat16
VMEM = pl.BlockSpec(memory_space=pltpu.VMEM)
SMEM = pl.BlockSpec(memory_space=pltpu.SMEM)


def dot(left, right):
    return jnp.dot(left, right, preferred_element_type=F32)


def dot_t(left, right):
    return lax.dot_general(left, right, (((1,), (1,)), ((), ())), preferred_element_type=F32)


def block_form(real_part, imag_part):
    top_rows = jnp.concatenate([real_part, imag_part], axis=1)
    bottom_rows = jnp.concatenate([-imag_part, real_part], axis=1)
    return jnp.concatenate([top_rows, bottom_rows], axis=0)


def factor(ref, level, side):
    return block_form(ref[level, side, 0], ref[level, side, 1])


def far_factor(ref, side):
    return block_form(ref[side, 0], ref[side, 1]).astype(BF16)


def split(value):
    high = value.astype(BF16)
    low = (value - high.astype(F32)).astype(BF16)
    return jnp.concatenate([high, low], axis=0)


def joined(product):
    rows = product.shape[0] // 2
    return product[:rows] + product[rows:]


def paired(ref):
    return jnp.concatenate([ref[0], ref[1]], axis=1)


def put(ref, value):
    ref[0] = value[:, :RANK]
    ref[1] = value[:, RANK:]


def flip_boxes(value, level):
    span = value.shape[0] // BOXES << level
    parts = [value[at : at + span] for at in range(0, value.shape[0], span)]
    return jnp.concatenate([parts[at ^ 1] for at in range(len(parts))], axis=0)


def cosine(step):
    half = math.sqrt(0.5)
    diagonal = jnp.where((step == 1) | (step == 7), F32(half), F32(-half))
    straight = jnp.where(step == 0, F32(1.0), jnp.where(step == 4, F32(-1.0), F32(0.0)))
    return jnp.where((step & 1) == 1, diagonal, straight)


def wave(freq):
    cos_values = [cosine((freq * time) & 7) for time in range(SAMPLES)]
    sin_values = [cosine((freq * time + 6) & 7) for time in range(SAMPLES)]
    return cos_values, sin_values


def local_forward(coeffs, factors):
    for level in range(LOCAL_LEVELS):
        parts = split(coeffs)
        own = joined(dot(parts, factor(factors, level, 0)))
        cross = joined(dot(parts, factor(factors, level, 1)))
        coeffs = own + flip_boxes(cross, level)
    return coeffs


def first_kernel(signal, freq, order, factors, *refs, groups):
    outs, spectrum = refs[:groups], refs[groups]
    shots = signal.shape[0]
    cos_values, sin_values = wave(freq[0])
    rows = lax.broadcasted_iota(jnp.int32, (SAMPLES, 1), 0)
    cos_column = jnp.zeros((SAMPLES, 1), F32)
    sin_column = jnp.zeros((SAMPLES, 1), F32)
    for time in range(SAMPLES):
        cos_column = jnp.where(rows == time, cos_values[time], cos_column)
        sin_column = jnp.where(rows == time, -sin_values[time], sin_column)
    for shot in range(shots):
        value = signal[shot]
        spectrum[shot : shot + 1, :] = jnp.sum(value * cos_column, axis=0, keepdims=True)
        spectrum[shots + shot : shots + shot + 1, :] = jnp.sum(
            value * sin_column, axis=0, keepdims=True
        )
    parts = split(spectrum[...])
    elements = parts.shape[1]
    element = lax.broadcasted_iota(jnp.int32, (elements, 2 * RANK), 0)
    size = shots // groups

    @pl.loop(0, BOXES // 2)
    def _(pair):
        start = pl.multiple_of(pair * 2 * RANK, 2 * RANK)
        place = order[:, pl.ds(start, 2 * RANK)]
        chosen = jnp.where(element == place, F32(1.0), F32(0.0)).astype(BF16)
        placed = joined(dot(parts, chosen))
        for half in range(2):
            lanes = slice(half * RANK, (half + 1) * RANK)
            rows = pl.ds(pl.multiple_of((2 * pair + half) * size, size), size)
            for group, out in enumerate(outs):
                out[0, rows, :] = placed[group * size : (group + 1) * size, lanes]
                out[1, rows, :] = placed[shots + group * size : shots + (group + 1) * size, lanes]

    for out in outs:
        put(out, local_forward(paired(out), factors))


def core_kernel(own, other, factors, out):
    level = LOCAL_LEVELS
    put(
        out,
        joined(dot(split(paired(own)), factor(factors, level, 0)))
        + joined(dot(split(paired(other)), factor(factors, level, 1))),
    )


def two_levels(own, near, far, both, factors, far_factors, level):
    first = joined(dot(split(paired(own)), factor(factors, level, 0))) + joined(
        dot(split(paired(near)), factor(factors, level, 1))
    )
    second = joined(dot(split(paired(far)), far_factor(far_factors, 0))) + joined(
        dot(split(paired(both)), far_factor(far_factors, 1))
    )
    return joined(dot(split(first), factor(factors, level + 1, 0))) + joined(
        dot(split(second), factor(factors, level + 1, 1))
    )


def two_adjoints(coeffs, factors, far_factors, level, own, near, far, both):
    parts = split(coeffs)
    first = split(joined(dot_t(parts, factor(factors, level + 1, 0))))
    second = split(joined(dot_t(parts, factor(factors, level + 1, 1))))
    put(own, joined(dot_t(first, factor(factors, level, 0))))
    put(near, joined(dot_t(first, factor(factors, level, 1))))
    put(far, joined(dot_t(second, far_factor(far_factors, 0))))
    put(both, joined(dot_t(second, far_factor(far_factors, 1))))


def forward_kernel(own, near, far, both, factors, far_factors, out, *, level):
    put(out, two_levels(own, near, far, both, factors, far_factors, level))


def adjoint_kernel(a, b, c, d, factors, far_factors, own, near, far, both, *, level):
    coeffs = (paired(a) + paired(b)) + (paired(c) + paired(d))
    two_adjoints(coeffs, factors, far_factors, level, own, near, far, both)


def core_adjoint_kernel(a, b, c, d, factors, own, other):
    level = LOCAL_LEVELS
    parts = split((paired(a) + paired(b)) + (paired(c) + paired(d)))
    put(own, joined(dot_t(parts, factor(factors, level, 0))))
    put(other, joined(dot_t(parts, factor(factors, level, 1))))


def local_adjoint_kernel(own, other, factors, out):
    coeffs = paired(own) + paired(other)
    for level in reversed(range(LOCAL_LEVELS)):
        parts = split(coeffs)
        cross = joined(dot_t(parts, factor(factors, level, 1)))
        coeffs = joined(dot_t(parts, factor(factors, level, 0))) + flip_boxes(cross, level)
    put(out, coeffs)


def image_kernel(
    own0, near0, far0, both0, factors, far_factors, weights, reflect, coupling,
    own, near, far, both,
    coeffs, stacked, scaled, field, total,
    *, level, shots,
):
    entered = two_levels(own0, near0, far0, both0, factors, far_factors, level)
    put(coeffs, entered)
    lanes = 2 * RANK
    for shot in range(shots):
        real = coeffs[0, pl.ds(shot, BOXES, stride=shots), :]
        imag = coeffs[1, pl.ds(shot, BOXES, stride=shots), :]
        rows = jnp.concatenate([real, imag], axis=1)
        turned = jnp.concatenate([-imag, real], axis=1)
        stacked[:, shot * lanes : (shot + 1) * lanes] = jnp.concatenate(
            [rows, turned], axis=0
        ).astype(BF16)
    total[...] = jnp.zeros_like(total)
    couple = block_form(coupling[0], coupling[1])
    block = Q_BLOCK

    @pl.loop(0, weights.shape[1] // block)
    def _(turn):
        start = pl.multiple_of(turn * block, block)
        weight = weights[:, pl.ds(start, block)]
        weight_t = weight.astype(F32).T.astype(BF16)
        rho = reflect[pl.ds(start, block), :].astype(F32)
        rho = jnp.concatenate([rho, rho], axis=1)
        for shot in range(shots):
            at = slice(shot * block, (shot + 1) * block)
            value = dot(weight_t, stacked[:, shot * lanes : (shot + 1) * lanes])
            field[at, :] = value
            scaled[at, :] = (rho * value).astype(BF16)
        coupled = dot(scaled[...], couple)
        for shot in range(shots):
            at = slice(shot * block, (shot + 1) * block)
            echo = (rho * (field[at, :] + coupled[at])).astype(BF16)
            total[:, shot * lanes : (shot + 1) * lanes] += dot(weight, echo)

    for shot in range(shots):
        real = total[:BOXES, shot * lanes : (shot + 1) * lanes]
        imag = total[BOXES:, shot * lanes : (shot + 1) * lanes]
        coeffs[0, pl.ds(shot, BOXES, stride=shots), :] = real[:, :RANK] + imag[:, RANK:]
        coeffs[1, pl.ds(shot, BOXES, stride=shots), :] = real[:, RANK:] - imag[:, :RANK]
    two_adjoints(paired(coeffs), factors, far_factors, level, own, near, far, both)


def time_samples(real, imag):
    (r1, r2, r3), (i1, i2, i3) = real, imag
    half = F32(math.sqrt(0.5))
    r13, r_13, i13, i_13 = r1 + r3, r1 - r3, i1 + i3, i1 - i3
    odd = half * (r_13 - i13)
    even = half * (r_13 + i13)
    return (
        r2 + r13, odd - i2, -r2 - i_13, i2 - even,
        r2 - r13, -odd - i2, i_13 - r2, even + i2,
    )


def summed_kernel(*refs, shots, group, last):
    *before, out, energy = refs[8:]
    spectra = refs[:4]
    freqs = [freq[0] for freq in refs[4:8]]
    chosen = [[jnp.where(freq == k, F32(1.0), F32(0.0)) for freq in freqs] for k in (1, 2, 3)]

    def one_box(box, power):
        rows = pl.ds(pl.multiple_of(box * shots, shots), shots)
        sums = []
        for part in range(2):
            values = [spectrum[part, rows, :] for spectrum in spectra]
            for weights in chosen:
                terms = [weight * value for weight, value in zip(weights, values)]
                sums.append((terms[0] + terms[1]) + (terms[2] + terms[3]))
        for value in sums:
            power = power + value * value
        for time, value in enumerate(time_samples(sums[:3], sums[3:])):
            if last:
                out[box, pl.ds(time, shots, stride=SAMPLES), :] = value
            else:
                out[time, rows, :] = value
        return power

    power = lax.fori_loop(0, BOXES, one_box, jnp.zeros((shots, RANK), F32))
    column = jnp.sum(power, axis=1, keepdims=True) * (SAMPLES / 2)
    at_shot = lax.broadcasted_iota(jnp.int32, (shots, RANK), 0)
    at_lane = lax.broadcasted_iota(jnp.int32, (shots, RANK), 1)
    mine = at_shot + group * shots == at_lane
    row = jnp.sum(jnp.where(mine, column, F32(0.0)), axis=0, keepdims=True)
    energy[...] = sum((ref[...] for ref in before), jnp.broadcast_to(row, energy.shape))


def amplitude(energy, clip_level, shots, group):
    row = jnp.sum(energy[...], axis=0, keepdims=True)
    count = clip_level.shape[1]
    root_mean = jnp.sqrt(row / (SAMPLES * ELEMENTS) + 1e-6)[:, :count]
    row = (4.0 + clip_level[...].astype(F32)) / 10.0 * root_mean
    at_shot = lax.broadcasted_iota(jnp.int32, (shots, count), 0)
    at_lane = lax.broadcasted_iota(jnp.int32, (shots, count), 1)
    mine = at_shot + group * shots == at_lane
    return jnp.sum(jnp.where(mine, row, F32(0.0)), axis=1, keepdims=True)


def next_kernel(summed, energy, clip_level, freq, factors, out, *, shots, group):
    amp = jnp.broadcast_to(amplitude(energy, clip_level, shots, group), (shots, RANK))
    inverse = 1.0 / amp
    cos_values, sin_values = wave(freq[0])

    @pl.loop(0, BOXES)
    def _(box):
        rows = pl.ds(pl.multiple_of(box * shots, shots), shots)
        real = jnp.zeros((shots, RANK), F32)
        imag = jnp.zeros((shots, RANK), F32)
        for time in range(SAMPLES):
            value = jnp.clip(summed[time, rows, :], -amp, amp)
            real = real + value * cos_values[time]
            imag = imag - value * sin_values[time]
        out[0, rows, :] = real * inverse
        out[1, rows, :] = imag * inverse

    put(out, local_forward(paired(out), factors))


def order_kernel(summed, order, out):
    left = jnp.concatenate([summed[box] for box in range(BOXES)], axis=1)
    parts = split(left)
    elements = parts.shape[1]
    element = lax.broadcasted_iota(jnp.int32, (2 * RANK, elements), 0)

    @pl.loop(0, elements // (2 * RANK))
    def _(tile):
        start = pl.multiple_of(tile * 2 * RANK, 2 * RANK)
        chosen = jnp.where(order[...] == element + start, F32(1.0), F32(0.0))
        out[:, pl.ds(start, 2 * RANK)] = joined(dot_t(parts, chosen.astype(BF16)))


def clip_kernel(*refs, shots, groups):
    energy, clip_level, out = refs[groups:]
    for group in range(groups):
        summed = refs[group]
        amp = amplitude(energy, clip_level, shots, group)
        for shot in range(shots):
            limit = jnp.broadcast_to(amp[shot : shot + 1, :], (SAMPLES, 1))
            value = summed[shot * SAMPLES : (shot + 1) * SAMPLES, :]
            out[group * shots + shot] = jnp.clip(value, -limit, limit) / limit


def call(
    body, outs, operands, smem=(), after=(), scratch=(), limit=24, flops=0, name=None, **settings
):
    count = len(operands)

    def kernel(*refs):
        body(*refs[:count], *refs[count + len(after) :], **settings)

    return pl.pallas_call(
        kernel,
        out_shape=outs,
        in_specs=[SMEM if at in smem else VMEM for at in range(count)]
        + [pl.BlockSpec(memory_space=pl.ANY)] * len(after),
        out_specs=jax.tree.map(lambda _: VMEM, outs),
        scratch_shapes=list(scratch),
        compiler_params=pltpu.CompilerParams(vmem_limit_bytes=limit << 20),
        cost_estimate=pl.CostEstimate(flops=flops, transcendentals=0, bytes_accessed=1 << 20),
        name=name,
    )(*operands, *after)


def exchange(values, axis):
    received = []
    for step, value in enumerate(values, 1):
        pairs = [(source, source ^ step) for source in range(lax.axis_size(axis))]
        received.append(lax.ppermute(value, axis, pairs))
    return received


def on_device(
    excitation,
    freq_index,
    elem_order,
    level_factors,
    image_weights,
    coupling,
    reflectivity,
    clip_level,
):
    shots = excitation.shape[0] // GROUPS
    rows = shots * BOXES
    leaves = lax.axis_size(LEAF)
    factors = level_factors[0, 0]
    weights = image_weights[0].reshape(2 * BOXES, image_weights.shape[3])
    couple = coupling[0]
    clips = clip_level.reshape(1, shots * GROUPS)
    coeff = jax.ShapeDtypeStruct((2, rows, RANK), F32)
    freqs = [freq_index] + exchange([freq_index] * 3, "band")

    def far_level(level, axis):
        pairs = [(source, source ^ 2) for source in range(lax.axis_size(axis))]
        return lax.ppermute(factors[level].astype(F32), axis, pairs)

    far_z = far_level(5, "leaf_1")
    far_x = far_level(7, "leaf_0")
    started = call(
        first_kernel,
        (coeff,) * GROUPS,
        (excitation, freq_index, elem_order, factors),
        smem=(1,),
        scratch=[pltpu.VMEM((2 * excitation.shape[0], excitation.shape[2]), F32)],
        flops=8_000_000_000,
        name="first",
        groups=GROUPS,
    )

    def levels_up(coeffs, after):
        (other,) = exchange([coeffs], "leaf_2")
        coeffs = call(core_kernel, coeff, (coeffs, other, factors), flops=500_000_000, name="core")
        received = exchange([coeffs] * 3, "leaf_1")
        coeffs = call(
            forward_kernel,
            coeff,
            (coeffs, *received, factors, far_z),
            after=after,
            flops=1_000_000_000,
            name="forward",
            level=5,
        )
        received = exchange([coeffs] * 3, "leaf_0")
        return call(
            image_kernel,
            (coeff,) * 4,
            (coeffs, *received, factors, far_x, weights, reflectivity, couple),
            scratch=[
                pltpu.VMEM((2, rows, RANK), F32),
                pltpu.VMEM((2 * BOXES, shots * 2 * RANK), BF16),
                pltpu.VMEM((shots * Q_BLOCK, 2 * RANK), BF16),
                pltpu.VMEM((shots * Q_BLOCK, 2 * RANK), F32),
                pltpu.VMEM((2 * BOXES, shots * 2 * RANK), F32),
            ],
            limit=36,
            flops=8_000_000_000,
            name="image",
            level=7,
            shots=shots,
        )

    def levels_down(own, sent):
        own, *sent = call(
            adjoint_kernel,
            (coeff,) * 4,
            (own, *exchange(sent, "leaf_0"), factors, far_z),
            flops=1_000_000_000,
            name="adjoint",
            level=5,
        )
        own, sent = call(
            core_adjoint_kernel,
            (coeff,) * 2,
            (own, *exchange(sent, "leaf_1"), factors),
            flops=500_000_000,
            name="core_adjoint",
        )
        (other,) = exchange([sent], "leaf_2")
        return call(
            local_adjoint_kernel,
            coeff,
            (own, other, factors),
            flops=1_000_000_000,
            name="local_adjoint",
        )

    def band_sum(spectrum, group, before, last):
        received = exchange([spectrum] * 3, "band")
        shape = (BOXES, shots * SAMPLES, RANK) if last else (SAMPLES, rows, RANK)
        return call(
            summed_kernel,
            (jax.ShapeDtypeStruct(shape, F32), jax.ShapeDtypeStruct((leaves, RANK), F32)),
            (spectrum, *received, *freqs, *before),
            smem=(4, 5, 6, 7),
            flops=1_000_000_000,
            name="summed",
            shots=shots,
            group=group,
            last=last,
        )

    for iteration in range(ITERS):
        last = iteration == ITERS - 1
        sums = []
        before = []
        for group, coeffs in enumerate(started):
            own, *sent = levels_up(coeffs, [] if iteration + group else freqs[1:])
            summed, energy = band_sum(levels_down(own, sent), group, before, last)
            sums.append(summed)
            before = [energy]
        energy = lax.all_to_all(energy, LEAF, 0, 0, tiled=True)
        if not last:
            started = [
                call(
                    next_kernel,
                    coeff,
                    (summed, energy, clips, freq_index, factors),
                    smem=(3,),
                    flops=1_000_000_000,
                    name="next",
                    shots=shots,
                    group=group,
                )
                for group, summed in enumerate(sums)
            ]
    ordered = [
        call(
            order_kernel,
            jax.ShapeDtypeStruct((shots * SAMPLES, excitation.shape[2]), F32),
            (summed, elem_order),
            flops=3_000_000_000,
            name="order",
        )
        for summed in sums
    ]
    return call(
        clip_kernel,
        jax.ShapeDtypeStruct(excitation.shape, F32),
        (*ordered, energy, clips),
        flops=500_000_000,
        name="clip",
        shots=shots,
        groups=GROUPS,
    )


def solution(mesh):
    finer = Mesh(
        mesh.devices.reshape(4, 4, 2, mesh.shape["band"]), ("leaf_0", "leaf_1", "leaf_2", "band")
    )
    placed = (
        P(None, None, LEAF),
        P("band"),
        P(LEAF, None),
        P("band", LEAF, None, None, None, None, None),
        P("band", None, None, LEAF),
        P("band", None, None, None),
        P(LEAF, None),
        P(),
    )
    return jax.shard_map(
        on_device, mesh=finer, in_specs=placed, out_specs=P(None, None, LEAF), check_vma=False
    )
```

```python
import math

import jax
import jax.numpy as jnp
from jax import lax
from jax.experimental import pallas as pl
from jax.experimental.pallas import tpu as pltpu
from jax.sharding import Mesh
from jax.sharding import PartitionSpec as P

ELEMENTS = 65536
ITERS = 2
RANK = 128
BOXES = 16
LOCAL_LEVELS = 4
SAMPLES = 8
Q_BLOCK = 512
GROUPS = 2
LEAF = ("leaf_0", "leaf_1", "leaf_2")
F32 = jnp.float32
BF16 = jnp.bfloat16
VMEM = pl.BlockSpec(memory_space=pltpu.VMEM)
RAW = pl.BlockSpec(memory_space=pl.ANY)


def dot(left, right):
    return jnp.dot(left, right, preferred_element_type=F32)


def dot_t(left, right):
    return lax.dot_general(left, right, (((1,), (1,)), ((), ())), preferred_element_type=F32)


def block_form(real_part, imag_part):
    top_rows = jnp.concatenate([real_part, imag_part], axis=1)
    bottom_rows = jnp.concatenate([-imag_part, real_part], axis=1)
    return jnp.concatenate([top_rows, bottom_rows], axis=0)


def factor(ref, level, side):
    return block_form(ref[level, side, 0], ref[level, side, 1])


def far_factor(ref, side):
    return block_form(ref[2 + 2 * side], ref[3 + 2 * side]).astype(BF16)


def put_with_factors(ref, value, factors, level):
    put(ref, value)
    for side in range(2):
        for part in range(2):
            ref[2 + 2 * side + part] = factors[level, side, part].astype(F32)


def split(value):
    high = value.astype(BF16)
    low = (value - high.astype(F32)).astype(BF16)
    return jnp.concatenate([high, low], axis=0)


def joined(product):
    rows = product.shape[0] // 2
    return product[:rows] + product[rows:]


def paired(ref):
    return jnp.concatenate([ref[0], ref[1]], axis=1)


def put(ref, value):
    ref[0] = value[:, :RANK]
    ref[1] = value[:, RANK:]


def flip_boxes(value, level):
    span = value.shape[0] // BOXES << level
    parts = [value[at : at + span] for at in range(0, value.shape[0], span)]
    return jnp.concatenate([parts[at ^ 1] for at in range(len(parts))], axis=0)


def cosine(step):
    step = step & 7
    half = math.sqrt(0.5)
    diagonal = jnp.where((step == 1) | (step == 7), F32(half), F32(-half))
    straight = jnp.where(step == 0, F32(1.0), jnp.where(step == 4, F32(-1.0), F32(0.0)))
    return jnp.where((step & 1) == 1, diagonal, straight)


def local_forward(coeffs, factors):
    for level in range(LOCAL_LEVELS):
        parts = split(coeffs)
        own = joined(dot(parts, factor(factors, level, 0)))
        cross = joined(dot(parts, factor(factors, level, 1)))
        coeffs = own + flip_boxes(cross, level)
    return coeffs


def first_kernel(
    signal_in, order_in, factors_in, freq, out, signal, order, factors, spectrum, coeffs, sems
):
    copies = [
        pltpu.make_async_copy(source, target, sems.at[at])
        for at, (source, target) in enumerate(
            (
                (signal_in, signal),
                (order_in, order),
                (factors_in.at[pl.ds(0, LOCAL_LEVELS)], factors),
            )
        )
    ]
    for copy in copies:
        copy.start()
    step = freq[...] * lax.broadcasted_iota(jnp.int32, freq.shape, 0)
    cos_column = cosine(step)[:, :1]
    sin_column = -cosine(step + 6)[:, :1]
    shots = signal.shape[0]
    copies[0].wait()

    @pl.loop(0, shots // SAMPLES)
    def _(part):
        start = pl.multiple_of(part * SAMPLES, SAMPLES)
        for sign, column in ((0, cos_column), (1, sin_column)):
            sums = [
                jnp.sum(signal[start + at] * column, axis=0, keepdims=True)
                for at in range(SAMPLES)
            ]
            spectrum[pl.ds(sign * shots + start, SAMPLES), :] = jnp.concatenate(sums, axis=0)

    copies[1].wait()
    parts = split(spectrum[...])
    elements = parts.shape[1]
    element = lax.broadcasted_iota(jnp.int32, (elements, RANK), 0)

    @pl.loop(0, BOXES)
    def _(box):
        place = order[:, pl.ds(pl.multiple_of(box * RANK, RANK), RANK)]
        chosen = jnp.where(element == place, F32(1.0), F32(0.0)).astype(BF16)
        placed = joined(dot(parts, chosen))
        rows = pl.ds(pl.multiple_of(box * shots, shots), shots)
        coeffs[0, rows, :] = placed[:shots]
        coeffs[1, rows, :] = placed[shots:]

    copies[2].wait()
    put(out, local_forward(paired(coeffs), factors))


def core_kernel(own, other, factors, *outs, groups):
    level = LOCAL_LEVELS
    outs, carriers = outs[:groups], outs[groups:]
    size = outs[0].shape[1] // BOXES
    shots = size * len(outs)
    coeffs = joined(dot(split(paired(own)), factor(factors, level, 0))) + joined(
        dot(split(paired(other)), factor(factors, level, 1))
    )
    for group, out in enumerate(outs):
        starts = [box * shots + group * size for box in range(BOXES)]
        part = jnp.concatenate([coeffs[at : at + size] for at in starts], axis=0)
        put(out, part)
        if group == 0:
            for carrier in carriers:
                put_with_factors(carrier, part, factors, level + 1)


def two_levels(own, near, far, both, factors, far_factors, level):
    first = joined(dot(split(paired(own)), factor(factors, level, 0))) + joined(
        dot(split(paired(near)), factor(factors, level, 1))
    )
    second = joined(dot(split(paired(far)), far_factor(far_factors, 0))) + joined(
        dot(split(paired(both)), far_factor(far_factors, 1))
    )
    return joined(dot(split(first), factor(factors, level + 1, 0))) + joined(
        dot(split(second), factor(factors, level + 1, 1))
    )


def two_adjoints(coeffs, factors, far_factors, level, own, near, far, both):
    parts = split(coeffs)
    first = split(joined(dot_t(parts, factor(factors, level + 1, 0))))
    second = split(joined(dot_t(parts, factor(factors, level + 1, 1))))
    put(own, joined(dot_t(first, factor(factors, level, 0))))
    put(near, joined(dot_t(first, factor(factors, level, 1))))
    put(far, joined(dot_t(second, far_factor(far_factors, 0))))
    put(both, joined(dot_t(second, far_factor(far_factors, 1))))


def forward_kernel(own, near, far, both, factors, far_factors, out, *carriers, level):
    coeffs = two_levels(own, near, far, both, factors, far_factors, level)
    put(out, coeffs)
    for carrier in carriers:
        put_with_factors(carrier, coeffs, factors, level + 2)


def adjoint_kernel(a, b, c, d, factors, far_factors, own, near, far, both, *, level):
    coeffs = (paired(a) + paired(b)) + (paired(c) + paired(d))
    two_adjoints(coeffs, factors, far_factors, level, own, near, far, both)


def core_adjoint_kernel(a, b, c, d, factors, own, other):
    level = LOCAL_LEVELS
    parts = split((paired(a) + paired(b)) + (paired(c) + paired(d)))
    put(own, joined(dot_t(parts, factor(factors, level, 0))))
    put(other, joined(dot_t(parts, factor(factors, level, 1))))


def local_adjoint_kernel(own, other, factors, freq, out):
    coeffs = paired(own) + paired(other)
    for level in reversed(range(LOCAL_LEVELS)):
        parts = split(coeffs)
        cross = joined(dot_t(parts, factor(factors, level, 1)))
        coeffs = joined(dot_t(parts, factor(factors, level, 0))) + flip_boxes(cross, level)
    rows = coeffs.shape[0]
    out[:rows, :] = coeffs[:, :RANK]
    out[rows : 2 * rows, :] = coeffs[:, RANK:]
    out[2 * rows :, :] = freq[...].astype(F32)


def image_kernel(
    own0, near0, far0, both0, factors, far_factors, weights, reflect, coupling,
    own, near, far, both,
    coeffs, stacked, echo, total,
    *, level, shots,
):
    entered = two_levels(own0, near0, far0, both0, factors, far_factors, level)
    put(coeffs, entered)
    lanes = 2 * RANK

    @pl.loop(0, shots)
    def _(shot):
        real = coeffs[0, pl.ds(shot, BOXES, stride=shots), :]
        imag = coeffs[1, pl.ds(shot, BOXES, stride=shots), :]
        rows = jnp.concatenate([real, imag], axis=1)
        turned = jnp.concatenate([-imag, real], axis=1)
        at = pl.ds(pl.multiple_of(shot * lanes, lanes), lanes)
        stacked[:, at] = jnp.concatenate([rows, turned], axis=0).astype(BF16)

    total[...] = jnp.zeros_like(total)
    couple = block_form(coupling[0], coupling[1])
    block = Q_BLOCK

    @pl.loop(0, weights.shape[1] // block)
    def _(turn):
        start = pl.multiple_of(turn * block, block)
        weight = weights[:, pl.ds(start, block)]
        weight_t = weight.astype(F32).T.astype(BF16)
        rho = reflect[pl.ds(start, block), :].astype(F32)
        rho = jnp.concatenate([rho, rho], axis=1)
        for shot in range(shots):
            at = slice(shot * lanes, (shot + 1) * lanes)
            field = dot(weight_t, stacked[:, at])
            coupled = dot((rho * field).astype(BF16), couple)
            echo[:, at] = (rho * (field + coupled)).astype(BF16)
        total[...] += dot(weight, echo[...])

    @pl.loop(0, shots)
    def _(shot):
        at = pl.ds(pl.multiple_of(shot * lanes, lanes), lanes)
        real, imag = total[:BOXES, at], total[BOXES:, at]
        rows = pl.ds(shot, BOXES, stride=shots)
        coeffs[0, rows, :] = real[:, :RANK] + imag[:, RANK:]
        coeffs[1, rows, :] = real[:, RANK:] - imag[:, :RANK]

    two_adjoints(paired(coeffs), factors, far_factors, level, own, near, far, both)


def time_samples(real, imag):
    (r1, r2, r3), (i1, i2, i3) = real, imag
    half = F32(math.sqrt(0.5))
    r13, r_13, i13, i_13 = r1 + r3, r1 - r3, i1 + i3, i1 - i3
    odd = half * (r_13 - i13)
    even = half * (r_13 + i13)
    return (
        r2 + r13, odd - i2, -r2 - i_13, i2 - even,
        r2 - r13, -odd - i2, i_13 - r2, even + i2,
    )


def summed_kernel(*refs, shots, group, last):
    *before, out, energy = refs[4:]
    spectra = refs[:4]
    count = shots * BOXES
    freqs = [
        jnp.broadcast_to(spectrum[2 * count : 2 * count + 1, :], (shots, RANK))
        for spectrum in spectra
    ]
    chosen = [
        [jnp.where(jnp.abs(freq - k) < 0.5, F32(1.0), F32(0.0)) for freq in freqs]
        for k in (1, 2, 3)
    ]

    def one_box(box, power):
        rows = pl.ds(pl.multiple_of(box * shots, shots), shots)
        sums = []
        for part in range(2):
            start = pl.multiple_of(part * count + box * shots, shots)
            values = [spectrum[pl.ds(start, shots), :] for spectrum in spectra]
            for weights in chosen:
                terms = [weight * value for weight, value in zip(weights, values)]
                sums.append((terms[0] + terms[1]) + (terms[2] + terms[3]))
        for value in sums:
            power = power + value * value
        for time, value in enumerate(time_samples(sums[:3], sums[3:])):
            if last:
                out[box, pl.ds(time, shots, stride=SAMPLES), :] = value
            else:
                out[time, rows, :] = value
        return power

    power = lax.fori_loop(0, BOXES, one_box, jnp.zeros((shots, RANK), F32))
    column = jnp.sum(power, axis=1, keepdims=True) * (SAMPLES / 2)
    at_shot = lax.broadcasted_iota(jnp.int32, (shots, RANK), 0)
    at_lane = lax.broadcasted_iota(jnp.int32, (shots, RANK), 1)
    mine = at_shot + group * shots == at_lane
    row = jnp.sum(jnp.where(mine, column, F32(0.0)), axis=0, keepdims=True)
    energy[...] = sum((ref[...] for ref in before), jnp.broadcast_to(row, energy.shape))


def amplitude(energy, clip_level, shots, group):
    row = jnp.sum(energy[...], axis=0, keepdims=True)
    count = clip_level.shape[1]
    root_mean = jnp.sqrt(row / (SAMPLES * ELEMENTS) + 1e-6)[:, :count]
    row = (4.0 + clip_level[...].astype(F32)) / 10.0 * root_mean
    at_shot = lax.broadcasted_iota(jnp.int32, (shots, count), 0)
    at_lane = lax.broadcasted_iota(jnp.int32, (shots, count), 1)
    mine = at_shot + group * shots == at_lane
    return jnp.sum(jnp.where(mine, row, F32(0.0)), axis=1, keepdims=True)


def next_kernel(*refs, shots, groups):
    energy, clip_level, freq, factors = refs[groups : groups + 4]
    out, coeffs = refs[groups + 4 :]
    step = jnp.broadcast_to(freq[:1, :], (shots, RANK))
    cos_values = [cosine(step * time) for time in range(SAMPLES)]
    sin_values = [cosine(step * time + 6) for time in range(SAMPLES)]
    for group, summed in enumerate(refs[:groups]):
        amp = amplitude(energy, clip_level, shots, group)
        amp = jnp.broadcast_to(amp, (shots, RANK))
        inverse = 1.0 / amp

        @pl.loop(0, BOXES)
        def _(box):
            rows = pl.ds(pl.multiple_of(box * shots, shots), shots)
            into = pl.ds(pl.multiple_of((box * groups + group) * shots, shots), shots)
            real = jnp.zeros((shots, RANK), F32)
            imag = jnp.zeros((shots, RANK), F32)
            for time in range(SAMPLES):
                value = jnp.clip(summed[time, rows, :], -amp, amp)
                real = real + value * cos_values[time]
                imag = imag - value * sin_values[time]
            coeffs[0, into, :] = real * inverse
            coeffs[1, into, :] = imag * inverse

    put(out, local_forward(paired(coeffs), factors))


def order_kernel(*refs):
    *sums, order, out = refs
    rows = [jnp.concatenate([ref[box] for box in range(BOXES)], axis=1) for ref in sums]
    parts = split(jnp.concatenate(rows, axis=0))
    elements = parts.shape[1]
    element = lax.broadcasted_iota(jnp.int32, (RANK, elements), 0)

    @pl.loop(0, elements // (RANK))
    def _(tile):
        start = pl.multiple_of(tile * RANK, RANK)
        chosen = jnp.where(order[...] == element + start, F32(1.0), F32(0.0))
        out[:, pl.ds(start, RANK)] = joined(dot_t(parts, chosen.astype(BF16)))


def clip_kernel(summed, energy, clip_level, out, *, shots):
    amp = amplitude(energy, clip_level, shots, 0)
    for shot in range(shots):
        limit = jnp.broadcast_to(amp[shot : shot + 1, :], (SAMPLES, 1))
        value = summed[shot * SAMPLES : (shot + 1) * SAMPLES, :]
        out[shot] = jnp.clip(value, -limit, limit) / limit


def call(
    body, outs, operands, raw=0, scratch=(), limit=24, flops=0, name=None, **settings
):
    def kernel(*refs):
        body(*refs, **settings)

    return pl.pallas_call(
        kernel,
        out_shape=outs,
        in_specs=[RAW if at < raw else VMEM for at in range(len(operands))],
        out_specs=jax.tree.map(lambda _: VMEM, outs),
        scratch_shapes=list(scratch),
        compiler_params=pltpu.CompilerParams(vmem_limit_bytes=limit << 20),
        cost_estimate=pl.CostEstimate(flops=flops, transcendentals=0, bytes_accessed=1 << 20),
        name=name,
    )(*operands)


def exchange(values, axis):
    received = []
    for step, value in enumerate(values, 1):
        pairs = [(source, source ^ step) for source in range(lax.axis_size(axis))]
        received.append(lax.ppermute(value, axis, pairs))
    return received


def on_device(
    excitation,
    freq_index,
    elem_order,
    level_factors,
    image_weights,
    coupling,
    reflectivity,
    clip_level,
):
    shots = excitation.shape[0] // GROUPS
    rows = shots * BOXES
    leaves = lax.axis_size(LEAF)
    factors = level_factors[0, 0]
    weights = image_weights[0].reshape(2 * BOXES, image_weights.shape[3])
    couple = coupling[0]
    clips = clip_level.reshape(1, shots * GROUPS)
    coeff = jax.ShapeDtypeStruct((2, rows, RANK), F32)
    freq = jnp.broadcast_to(freq_index, (SAMPLES, RANK))
    every = shots * GROUPS
    whole = jax.ShapeDtypeStruct((2, every * BOXES, RANK), F32)
    rough = pltpu.VMEM((2, every * BOXES, RANK), F32)

    assert rows == RANK
    carrier = jax.ShapeDtypeStruct((6, rows, RANK), F32)
    far_levels = {}

    coeffs = call(
        first_kernel,
        whole,
        (excitation, elem_order, factors, freq),
        raw=3,
        scratch=[
            pltpu.VMEM(excitation.shape, F32),
            pltpu.VMEM(elem_order.shape, jnp.int32),
            pltpu.VMEM((LOCAL_LEVELS, *factors.shape[1:]), BF16),
            pltpu.VMEM((2 * every, excitation.shape[2]), F32),
            rough,
            pltpu.SemaphoreType.DMA((3,)),
        ],
        flops=8_000_000_000,
        name="first",
    )

    def gathered(coeffs, carriers, axis):
        far = carriers[0] if carriers else coeffs
        received = exchange([coeffs, far, coeffs], axis)
        far_levels.setdefault(axis, received[1])
        return received

    def levels_up(coeffs, carriers):
        received = gathered(coeffs, carriers, "leaf_1")
        coeffs, *carriers = call(
            forward_kernel,
            [coeff] + [carrier] * len(carriers),
            (coeffs, *received, factors, far_levels["leaf_1"]),
            flops=1_000_000_000,
            name="forward",
            level=5,
        )
        received = gathered(coeffs, carriers, "leaf_0")
        far_x = far_levels["leaf_0"]
        return call(
            image_kernel,
            (coeff,) * 4,
            (coeffs, *received, factors, far_x, weights, reflectivity, couple),
            scratch=[
                pltpu.VMEM((2, rows, RANK), F32),
                pltpu.VMEM((2 * BOXES, shots * 2 * RANK), BF16),
                pltpu.VMEM((Q_BLOCK, shots * 2 * RANK), BF16),
                pltpu.VMEM((2 * BOXES, shots * 2 * RANK), F32),
            ],
            limit=36,
            flops=8_000_000_000,
            name="image",
            level=7,
            shots=shots,
        )

    def levels_down(own, sent):
        own, *sent = call(
            adjoint_kernel,
            (coeff,) * 4,
            (own, *exchange(sent, "leaf_0"), factors, far_levels["leaf_1"]),
            flops=1_000_000_000,
            name="adjoint",
            level=5,
        )
        own, sent = call(
            core_adjoint_kernel,
            (coeff,) * 2,
            (own, *exchange(sent, "leaf_1"), factors),
            flops=500_000_000,
            name="core_adjoint",
        )
        (other,) = exchange([sent], "leaf_2")
        return call(
            local_adjoint_kernel,
            jax.ShapeDtypeStruct((2 * rows + SAMPLES, RANK), F32),
            (own, other, factors, freq),
            flops=1_000_000_000,
            name="local_adjoint",
        )

    def band_sum(spectrum, group, before, last):
        received = exchange([spectrum] * 3, "band")
        shape = (BOXES, shots * SAMPLES, RANK) if last else (SAMPLES, rows, RANK)
        return call(
            summed_kernel,
            (jax.ShapeDtypeStruct(shape, F32), jax.ShapeDtypeStruct((leaves, RANK), F32)),
            (spectrum, *received, *before),
            flops=1_000_000_000,
            name="summed",
            shots=shots,
            group=group,
            last=last,
        )

    for iteration in range(ITERS):
        last = iteration == ITERS - 1
        sums = []
        before = []
        (other,) = exchange([coeffs], "leaf_2")
        started = call(
            core_kernel,
            [coeff] * GROUPS + [carrier] * (iteration == 0),
            (coeffs, other, factors),
            flops=1_000_000_000,
            name="core",
            groups=GROUPS,
        )
        for group, coeffs in enumerate(started[:GROUPS]):
            own, *sent = levels_up(coeffs, started[GROUPS:] if group == 0 else [])
            summed, energy = band_sum(levels_down(own, sent), group, before, last)
            sums.append(summed)
            before = [energy]
        energy = lax.all_to_all(energy, LEAF, 0, 0, tiled=True)
        if not last:
            coeffs = call(
                next_kernel,
                whole,
                (*sums, energy, clips, freq, factors),
                scratch=[rough],
                flops=2_000_000_000,
                name="next",
                shots=shots,
                groups=GROUPS,
            )
    ordered = call(
        order_kernel,
        jax.ShapeDtypeStruct((every * SAMPLES, excitation.shape[2]), F32),
        (*sums, elem_order),
        flops=4_000_000_000,
        name="order",
    )
    return call(
        clip_kernel,
        jax.ShapeDtypeStruct(excitation.shape, F32),
        (ordered, energy, clips),
        flops=500_000_000,
        name="clip",
        shots=every,
    )


def solution(mesh):
    finer = Mesh(
        mesh.devices.reshape(4, 4, 2, mesh.shape["band"]), ("leaf_0", "leaf_1", "leaf_2", "band")
    )
    placed = (
        P(None, None, LEAF),
        P("band"),
        P(LEAF, None),
        P("band", LEAF, None, None, None, None, None),
        P("band", None, None, LEAF),
        P("band", None, None, None),
        P(LEAF, None),
        P(),
    )
    return jax.shard_map(
        on_device, mesh=finer, in_specs=placed, out_specs=P(None, None, LEAF), check_vma=False
    )
```

```python
import math

import jax
import jax.numpy as jnp
from jax import lax
from jax.experimental import pallas as pl
from jax.experimental.pallas import tpu as pltpu
from jax.sharding import Mesh
from jax.sharding import PartitionSpec as P


ELEMENTS = 65536
ITERS = 2
RANK = 128
BOXES = 16
LOCAL_LEVELS = 4
SAMPLES = 8
Q_BLOCK = 512
GROUPS = 2
LEAF = ("leaf_0", "leaf_1", "leaf_2")
LEAF_BAND = (*LEAF, "band")
F32 = jnp.float32
BF16 = jnp.bfloat16
VMEM = pl.BlockSpec(memory_space=pltpu.VMEM)
RAW = pl.BlockSpec(memory_space=pltpu.MemorySpace.HBM)


def dot(left, right):
    return jnp.dot(left, right, preferred_element_type=F32)


def dot_t(left, right):
    return lax.dot_general(left, right, (((1,), (1,)), ((), ())), preferred_element_type=F32)


def block_form(real_part, imag_part):
    top_rows = jnp.concatenate([real_part, imag_part], axis=1)
    bottom_rows = jnp.concatenate([-imag_part, real_part], axis=1)
    return jnp.concatenate([top_rows, bottom_rows], axis=0)


def factor(ref, level, side):
    return block_form(ref[level, side, 0], ref[level, side, 1])


def far_factor(ref, side):
    return block_form(ref[side, 0], ref[side, 1]).astype(BF16)


def split(value):
    high = value.astype(BF16)
    low = (value - high.astype(F32)).astype(BF16)
    return jnp.concatenate([high, low], axis=0)


def joined(product):
    rows = product.shape[0] // 2
    return product[:rows] + product[rows:]


def paired(ref):
    return jnp.concatenate([ref[0], ref[1]], axis=1)


def put(ref, value):
    ref[0] = value[:, :RANK]
    ref[1] = value[:, RANK:]


def flip_boxes(value, level):
    span = value.shape[0] // BOXES << level
    parts = [value[at : at + span] for at in range(0, value.shape[0], span)]
    return jnp.concatenate([parts[at ^ 1] for at in range(len(parts))], axis=0)


def cosine(step):
    step = step & 7
    half = math.sqrt(0.5)
    diagonal = jnp.where((step == 1) | (step == 7), F32(half), F32(-half))
    straight = jnp.where(step == 0, F32(1.0), jnp.where(step == 4, F32(-1.0), F32(0.0)))
    return jnp.where((step & 1) == 1, diagonal, straight)


def local_forward(coeffs, factors):
    for level in range(LOCAL_LEVELS):
        parts = split(coeffs)
        own = joined(dot(parts, factor(factors, level, 0)))
        cross = joined(dot(parts, factor(factors, level, 1)))
        coeffs = own + flip_boxes(cross, level)
    return coeffs


def first_kernel(
    signal_in, order_in, factors_in, freq, out, signal, order, factors, spectrum, coeffs, sems
):
    copies = [
        pltpu.make_async_copy(source, target, sems.at[at])
        for at, (source, target) in enumerate(
            (
                (signal_in, signal),
                (order_in, order),
                (factors_in.at[pl.ds(0, LOCAL_LEVELS)], factors),
            )
        )
    ]
    for copy in copies:
        copy.start()
    step = freq[...] * lax.broadcasted_iota(jnp.int32, freq.shape, 0)
    cos_column = cosine(step)[:, :1]
    sin_column = -cosine(step + 6)[:, :1]
    shots = signal.shape[0]
    copies[0].wait()

    @pl.loop(0, shots // SAMPLES)
    def _(part):
        start = pl.multiple_of(part * SAMPLES, SAMPLES)
        for sign, column in ((0, cos_column), (1, sin_column)):
            sums = [
                jnp.sum(signal[start + at] * column, axis=0, keepdims=True)
                for at in range(SAMPLES)
            ]
            spectrum[pl.ds(sign * shots + start, SAMPLES), :] = jnp.concatenate(sums, axis=0)

    copies[1].wait()
    parts = split(spectrum[...])
    elements = parts.shape[1]
    element = lax.broadcasted_iota(jnp.int32, (elements, RANK), 0)

    @pl.loop(0, BOXES)
    def _(box):
        place = order[:, pl.ds(pl.multiple_of(box * RANK, RANK), RANK)]
        chosen = jnp.where(element == place, F32(1.0), F32(0.0)).astype(BF16)
        placed = joined(dot(parts, chosen))
        rows = pl.ds(pl.multiple_of(box * shots, shots), shots)
        coeffs[0, rows, :] = placed[:shots]
        coeffs[1, rows, :] = placed[shots:]

    copies[2].wait()
    put(out, local_forward(paired(coeffs), factors))


def core_kernel(own, other, factors, *outs):
    level = LOCAL_LEVELS
    size = outs[0].shape[1] // BOXES
    shots = size * len(outs)
    coeffs = joined(dot(split(paired(own)), factor(factors, level, 0))) + joined(
        dot(split(paired(other)), factor(factors, level, 1))
    )
    for group, out in enumerate(outs):
        starts = [box * shots + group * size for box in range(BOXES)]
        put(out, jnp.concatenate([coeffs[at : at + size] for at in starts], axis=0))


def two_levels(own, near, far, both, factors, far_factors, level):
    first = joined(dot(split(paired(own)), factor(factors, level, 0))) + joined(
        dot(split(paired(near)), factor(factors, level, 1))
    )
    second = joined(dot(split(paired(far)), far_factor(far_factors, 0))) + joined(
        dot(split(paired(both)), far_factor(far_factors, 1))
    )
    return joined(dot(split(first), factor(factors, level + 1, 0))) + joined(
        dot(split(second), factor(factors, level + 1, 1))
    )


def two_adjoints(coeffs, factors, far_factors, level, own, near, far, both):
    parts = split(coeffs)
    first = split(joined(dot_t(parts, factor(factors, level + 1, 0))))
    second = split(joined(dot_t(parts, factor(factors, level + 1, 1))))
    put(own, joined(dot_t(first, factor(factors, level, 0))))
    put(near, joined(dot_t(first, factor(factors, level, 1))))
    put(far, joined(dot_t(second, far_factor(far_factors, 0))))
    put(both, joined(dot_t(second, far_factor(far_factors, 1))))


def forward_kernel(own, near, far, both, factors, far_factors, out, *, level):
    put(out, two_levels(own, near, far, both, factors, far_factors, level))


def adjoint_kernel(a, b, c, d, factors, far_factors, own, near, far, both, *, level):
    coeffs = (paired(a) + paired(b)) + (paired(c) + paired(d))
    two_adjoints(coeffs, factors, far_factors, level, own, near, far, both)


def core_adjoint_kernel(*refs):
    *terms, factors, own, other = refs
    level = LOCAL_LEVELS
    sums = []
    for at in range(0, len(terms), 4):
        a, b, c, d = (paired(ref) for ref in terms[at : at + 4])
        sums.append((a + b) + (c + d))
    size = sums[0].shape[0] // BOXES
    rows = [part[box * size : (box + 1) * size] for box in range(BOXES) for part in sums]
    parts = split(jnp.concatenate(rows, axis=0))
    put(own, joined(dot_t(parts, factor(factors, level, 0))))
    put(other, joined(dot_t(parts, factor(factors, level, 1))))


def local_adjoint_kernel(own, other, factors, freq, out, *quarters):
    coeffs = paired(own) + paired(other)
    for level in reversed(range(LOCAL_LEVELS)):
        parts = split(coeffs)
        cross = joined(dot_t(parts, factor(factors, level, 1)))
        coeffs = joined(dot_t(parts, factor(factors, level, 0))) + flip_boxes(cross, level)
    rows = coeffs.shape[0]
    out[:rows, :] = coeffs[:, :RANK]
    out[rows : 2 * rows, :] = coeffs[:, RANK:]
    out[2 * rows :, :] = freq[...].astype(F32)
    band = lax.axis_index("band")
    size = rows // len(quarters)
    for step, quarter in enumerate(quarters):
        start = pl.multiple_of((band ^ step) * size, size)
        quarter[:size, :] = out[pl.ds(start, size), :]
        quarter[size : 2 * size, :] = out[pl.ds(rows + start, size), :]
        quarter[2 * size :, :] = freq[...].astype(F32)


def image_kernel(
    own0, near0, far0, both0, factors, far_factors, weights, reflect, coupling,
    own, near, far, both,
    coeffs, stacked, echo, total,
    *, level, shots,
):
    entered = two_levels(own0, near0, far0, both0, factors, far_factors, level)
    put(coeffs, entered)
    lanes = 2 * RANK

    @pl.loop(0, shots)
    def _(shot):
        real = coeffs[0, pl.ds(shot, BOXES, stride=shots), :]
        imag = coeffs[1, pl.ds(shot, BOXES, stride=shots), :]
        rows = jnp.concatenate([real, imag], axis=1)
        turned = jnp.concatenate([-imag, real], axis=1)
        at = pl.ds(pl.multiple_of(shot * lanes, lanes), lanes)
        stacked[:, at] = jnp.concatenate([rows, turned], axis=0).astype(BF16)

    total[...] = jnp.zeros_like(total)
    couple = block_form(coupling[0], coupling[1])
    block = Q_BLOCK

    @pl.loop(0, weights.shape[1] // block)
    def _(turn):
        start = pl.multiple_of(turn * block, block)
        weight = weights[:, pl.ds(start, block)]
        weight_t = weight.astype(F32).T.astype(BF16)
        rho = reflect[pl.ds(start, block), :].astype(F32)
        rho = jnp.concatenate([rho, rho], axis=1)
        for shot in range(shots):
            at = slice(shot * lanes, (shot + 1) * lanes)
            field = dot(weight_t, stacked[:, at])
            coupled = dot((rho * field).astype(BF16), couple)
            echo[:, at] = (rho * (field + coupled)).astype(BF16)
        total[...] += dot(weight, echo[...])

    @pl.loop(0, shots)
    def _(shot):
        at = pl.ds(pl.multiple_of(shot * lanes, lanes), lanes)
        real, imag = total[:BOXES, at], total[BOXES:, at]
        rows = pl.ds(shot, BOXES, stride=shots)
        coeffs[0, rows, :] = real[:, :RANK] + imag[:, RANK:]
        coeffs[1, rows, :] = real[:, RANK:] - imag[:, :RANK]

    two_adjoints(paired(coeffs), factors, far_factors, level, own, near, far, both)


def time_samples(real, imag):
    (r1, r2, r3), (i1, i2, i3) = real, imag
    half = F32(math.sqrt(0.5))
    r13, r_13, i13, i_13 = r1 + r3, r1 - r3, i1 + i3, i1 - i3
    odd = half * (r_13 - i13)
    even = half * (r_13 + i13)
    return (
        r2 + r13, odd - i2, -r2 - i_13, i2 - even,
        r2 - r13, -odd - i2, i_13 - r2, even + i2,
    )


def frequency_sums(spectra, shots):
    count = (spectra[0].shape[0] - SAMPLES) // 2
    freqs = [
        jnp.broadcast_to(spectrum[2 * count : 2 * count + 1, :], (shots, RANK))
        for spectrum in spectra
    ]
    chosen = [
        [jnp.where(jnp.abs(freq - k) < 0.5, F32(1.0), F32(0.0)) for freq in freqs]
        for k in (1, 2, 3)
    ]

    def at_box(box):
        sums = []
        for part in range(2):
            start = pl.multiple_of(part * count + box * shots, shots)
            values = [spectrum[pl.ds(start, shots), :] for spectrum in spectra]
            for weights in chosen:
                terms = [weight * value for weight, value in zip(weights, values)]
                sums.append((terms[0] + terms[1]) + (terms[2] + terms[3]))
        return sums

    return at_box, count // shots


def energy_kernel(s0, s1, s2, s3, energy, *, shots):
    at_box, boxes = frequency_sums((s0, s1, s2, s3), shots)

    def one_box(box, power):
        return power + sum(value * value for value in at_box(box))

    power = lax.fori_loop(0, boxes, one_box, jnp.zeros((shots, RANK), F32))
    column = jnp.sum(power, axis=1, keepdims=True) * (SAMPLES / 2)
    at_shot = lax.broadcasted_iota(jnp.int32, (shots, RANK), 0)
    at_lane = lax.broadcasted_iota(jnp.int32, (shots, RANK), 1)
    row = jnp.sum(jnp.where(at_shot == at_lane, column, F32(0.0)), axis=0, keepdims=True)
    energy[...] = jnp.broadcast_to(row, energy.shape)


def summed_kernel(s0, s1, s2, s3, out, *, shots, last):
    at_box, boxes = frequency_sums((s0, s1, s2, s3), shots)

    @pl.loop(0, boxes)
    def _(box):
        sums = at_box(box)
        rows = pl.ds(pl.multiple_of(box * shots, shots), shots)
        for time, value in enumerate(time_samples(sums[:3], sums[3:])):
            if last:
                out[box, pl.ds(time, shots, stride=SAMPLES), :] = value
            else:
                out[time, rows, :] = value


def amplitude(energy, clip_level, shots):
    row = jnp.sum(energy[...], axis=0, keepdims=True)
    root_mean = jnp.sqrt(row / (SAMPLES * ELEMENTS) + 1e-6)[:, :shots]
    row = (4.0 + clip_level[...].astype(F32)) / 10.0 * root_mean
    at_shot = lax.broadcasted_iota(jnp.int32, (shots, shots), 0)
    at_lane = lax.broadcasted_iota(jnp.int32, (shots, shots), 1)
    return jnp.sum(jnp.where(at_shot == at_lane, row, F32(0.0)), axis=1, keepdims=True)


def next_kernel(summed, energy, clip_level, freq, factors, out, coeffs, *, shots):
    step = jnp.broadcast_to(freq[:1, :], (shots, RANK))
    cos_values = [cosine(step * time) for time in range(SAMPLES)]
    sin_values = [cosine(step * time + 6) for time in range(SAMPLES)]
    amp = jnp.broadcast_to(amplitude(energy, clip_level, shots), (shots, RANK))
    inverse = 1.0 / amp

    @pl.loop(0, BOXES)
    def _(box):
        rows = pl.ds(pl.multiple_of(box * shots, shots), shots)
        real = jnp.zeros((shots, RANK), F32)
        imag = jnp.zeros((shots, RANK), F32)
        for time in range(SAMPLES):
            value = jnp.clip(summed[time, rows, :], -amp, amp)
            real = real + value * cos_values[time]
            imag = imag - value * sin_values[time]
        coeffs[0, rows, :] = real * inverse
        coeffs[1, rows, :] = imag * inverse

    put(out, local_forward(paired(coeffs), factors))


def order_kernel(summed, order, out, column):
    @pl.loop(0, BOXES)
    def _(box):
        at = pl.ds(pl.multiple_of(box * RANK, RANK), RANK)
        column[at, :] = jnp.broadcast_to(order[:, at].astype(F32), (RANK, RANK)).T

    parts = split(jnp.concatenate([summed[box] for box in range(BOXES)], axis=1))
    elements = parts.shape[1]
    element = lax.broadcasted_iota(jnp.int32, (elements, RANK), 1).astype(F32)

    @pl.loop(0, elements // (2 * RANK))
    def _(tile):
        start = pl.multiple_of(tile * 2 * RANK, 2 * RANK)
        first = column[...] - start.astype(F32)
        halves = [
            jnp.where(first == element + offset, F32(1.0), F32(0.0)).astype(BF16)
            for offset in (0.0, float(RANK))
        ]
        out[:, pl.ds(start, 2 * RANK)] = joined(dot(parts, jnp.concatenate(halves, axis=1)))


def clip_kernel(summed, energy, clip_level, out, *, shots):
    amp = amplitude(energy, clip_level, shots)
    for shot in range(shots):
        limit = jnp.broadcast_to(amp[shot : shot + 1, :], (SAMPLES, 1))
        value = summed[shot * SAMPLES : (shot + 1) * SAMPLES, :]
        out[shot] = jnp.clip(value, -limit, limit) / limit


def call(body, outs, operands, raw=0, scratch=(), limit=24, flops=0, **settings):
    def kernel(*refs):
        body(*refs, **settings)

    return pl.pallas_call(
        kernel,
        out_shape=outs,
        in_specs=[RAW if at < raw else VMEM for at in range(len(operands))],
        out_specs=jax.tree.map(lambda _: VMEM, outs),
        scratch_shapes=list(scratch),
        compiler_params=pltpu.CompilerParams(vmem_limit_bytes=limit << 20),
        cost_estimate=pl.CostEstimate(flops=flops, transcendentals=0, bytes_accessed=1 << 20),
    )(*operands)


def exchange(values, axis):
    received = []
    for step, value in enumerate(values, 1):
        pairs = [(source, source ^ step) for source in range(lax.axis_size(axis))]
        received.append(lax.ppermute(value, axis, pairs))
    return received


def on_device(
    excitation,
    freq_index,
    elem_order,
    level_factors,
    image_weights,
    coupling,
    reflectivity,
    clip_level,
):
    shots = excitation.shape[0] // GROUPS
    rows = shots * BOXES
    leaves = lax.axis_size(LEAF)
    bands = lax.axis_size("band")
    factors = level_factors[0, 0]
    weights = image_weights[0].reshape(2 * BOXES, image_weights.shape[3])
    couple = coupling[0]
    clips = clip_level.reshape(1, shots * GROUPS)
    coeff = jax.ShapeDtypeStruct((2, rows, RANK), F32)
    freq = jnp.broadcast_to(freq_index, (SAMPLES, RANK))
    every = shots * GROUPS
    whole = jax.ShapeDtypeStruct((2, every * BOXES, RANK), F32)
    rough = pltpu.VMEM((2, every * BOXES, RANK), F32)


    def far_level(level, axis):
        pairs = [(source, source ^ 2) for source in range(lax.axis_size(axis))]
        return lax.ppermute(factors[level].astype(F32), axis, pairs)

    far_z = far_level(5, "leaf_1")
    far_x = far_level(7, "leaf_0")
    coeffs = call(
        first_kernel,
        whole,
        (excitation, elem_order, factors, freq),
        raw=3,
        scratch=[
            pltpu.VMEM(excitation.shape, F32),
            pltpu.VMEM(elem_order.shape, jnp.int32),
            pltpu.VMEM((LOCAL_LEVELS, *factors.shape[1:]), BF16),
            pltpu.VMEM((2 * every, excitation.shape[2]), F32),
            rough,
            pltpu.SemaphoreType.DMA((3,)),
        ],
        flops=8_000_000_000,
    )

    def levels_up(coeffs):
        received = exchange([coeffs] * 3, "leaf_1")
        coeffs = call(
            forward_kernel, coeff, (coeffs, *received, factors, far_z), flops=1_000_000_000, level=5
        )
        received = exchange([coeffs] * 3, "leaf_0")
        return call(
            image_kernel,
            (coeff,) * 4,
            (coeffs, *received, factors, far_x, weights, reflectivity, couple),
            scratch=[
                pltpu.VMEM((2, rows, RANK), F32),
                pltpu.VMEM((2 * BOXES, shots * 2 * RANK), BF16),
                pltpu.VMEM((Q_BLOCK, shots * 2 * RANK), BF16),
                pltpu.VMEM((2 * BOXES, shots * 2 * RANK), F32),
            ],
            limit=36,
            flops=8_000_000_000,
            level=7,
            shots=shots,
        )

    def levels_down(own, *sent):
        own, *sent = call(
            adjoint_kernel,
            (coeff,) * 4,
            (own, *exchange(sent, "leaf_0"), factors, far_z),
            flops=1_000_000_000,
            level=5,
        )
        return own, *exchange(sent, "leaf_1")

    for iteration in range(ITERS):
        last = iteration == ITERS - 1
        (other,) = exchange([coeffs], "leaf_2")
        started = call(
            core_kernel, (coeff,) * GROUPS, (coeffs, other, factors), flops=1_000_000_000
        )
        terms = []
        for coeffs in started:
            terms += levels_down(*levels_up(coeffs))
        own, sent = call(core_adjoint_kernel, (whole,) * 2, (*terms, factors), flops=1_000_000_000)
        (other,) = exchange([sent], "leaf_2")
        spectrum, *quarters = call(
            local_adjoint_kernel,
            [jax.ShapeDtypeStruct((2 * every * BOXES + SAMPLES, RANK), F32)]
            + [jax.ShapeDtypeStruct((2 * every * BOXES // bands + SAMPLES, RANK), F32)] * bands,
            (own, other, factors, freq),
            flops=2_000_000_000,
        )
        quarters = [quarters[0], *exchange(quarters[1:], "band")]
        energy = call(
            energy_kernel,
            jax.ShapeDtypeStruct((leaves * bands, RANK), F32),
            quarters,
            flops=200_000_000,
            shots=every,
        )
        energy = lax.all_to_all(energy, LEAF_BAND, 0, 0, tiled=True)
        spectra = [spectrum, *exchange([spectrum] * 3, "band")]
        shape = (BOXES, every * SAMPLES, RANK) if last else (SAMPLES, every * BOXES, RANK)
        summed = call(
            summed_kernel,
            jax.ShapeDtypeStruct(shape, F32),
            spectra,
            flops=1_000_000_000,
            shots=every,
            last=last,
        )
        if not last:
            coeffs = call(
                next_kernel,
                whole,
                (summed, energy, clips, freq, factors),
                scratch=[rough],
                flops=2_000_000_000,
                shots=every,
            )
    ordered = call(
        order_kernel,
        jax.ShapeDtypeStruct((every * SAMPLES, excitation.shape[2]), F32),
        (summed, elem_order),
        scratch=[pltpu.VMEM((excitation.shape[2], RANK), F32)],
        flops=4_000_000_000,
    )
    return call(
        clip_kernel,
        jax.ShapeDtypeStruct(excitation.shape, F32),
        (ordered, energy, clips),
        flops=500_000_000,
        shots=every,
    )


def solution(mesh):
    finer = Mesh(
        mesh.devices.reshape(4, 4, 2, mesh.shape["band"]), ("leaf_0", "leaf_1", "leaf_2", "band")
    )
    placed = (
        P(None, None, LEAF),
        P("band"),
        P(LEAF, None),
        P("band", LEAF, None, None, None, None, None),
        P("band", None, None, LEAF),
        P("band", None, None, None),
        P(LEAF, None),
        P(),
    )

    return jax.shard_map(
        on_device, mesh=finer, in_specs=placed, out_specs=P(None, None, LEAF), check_vma=False
    )
```

```python
import math

import jax
import jax.numpy as jnp
from jax import lax
from jax.experimental import pallas as pl
from jax.experimental.pallas import tpu as pltpu
from jax.sharding import Mesh
from jax.sharding import PartitionSpec as P


ELEMENTS = 65536
ITERS = 2
RANK = 128
BOXES = 16
LOCAL_LEVELS = 4
SAMPLES = 8
Q_BLOCK = 512
GROUPS = 2
LEAF = ("leaf_0", "leaf_1", "leaf_2")
F32 = jnp.float32
BF16 = jnp.bfloat16
VMEM = pl.BlockSpec(memory_space=pltpu.VMEM)
RAW = pl.BlockSpec(memory_space=pltpu.MemorySpace.HBM)


def dot(left, right):
    return jnp.dot(left, right, preferred_element_type=F32)


def dot_t(left, right):
    return lax.dot_general(left, right, (((1,), (1,)), ((), ())), preferred_element_type=F32)


def block_form(real_part, imag_part):
    top_rows = jnp.concatenate([real_part, imag_part], axis=1)
    bottom_rows = jnp.concatenate([-imag_part, real_part], axis=1)
    return jnp.concatenate([top_rows, bottom_rows], axis=0)


def factor(ref, level, side):
    return block_form(ref[level, side, 0], ref[level, side, 1])


def far_factor(ref, side):
    return block_form(ref[side, 0], ref[side, 1]).astype(BF16)


def split(value):
    high = value.astype(BF16)
    low = (value - high.astype(F32)).astype(BF16)
    return jnp.concatenate([high, low], axis=0)


def joined(product):
    rows = product.shape[0] // 2
    return product[:rows] + product[rows:]


def paired(ref):
    return jnp.concatenate([ref[0], ref[1]], axis=1)


def put(ref, value):
    ref[0] = value[:, :RANK]
    ref[1] = value[:, RANK:]


def flip_boxes(value, level):
    span = value.shape[0] // BOXES << level
    parts = [value[at : at + span] for at in range(0, value.shape[0], span)]
    return jnp.concatenate([parts[at ^ 1] for at in range(len(parts))], axis=0)


def cosine(step):
    step = step & 7
    half = math.sqrt(0.5)
    diagonal = jnp.where((step == 1) | (step == 7), F32(half), F32(-half))
    straight = jnp.where(step == 0, F32(1.0), jnp.where(step == 4, F32(-1.0), F32(0.0)))
    return jnp.where((step & 1) == 1, diagonal, straight)


def local_forward(coeffs, factors):
    for level in range(LOCAL_LEVELS):
        parts = split(coeffs)
        own = joined(dot(parts, factor(factors, level, 0)))
        cross = joined(dot(parts, factor(factors, level, 1)))
        coeffs = own + flip_boxes(cross, level)
    return coeffs


def first_kernel(
    signal_in, order_in, factors_in, freq, out, signal, order, factors, spectrum, coeffs, sems
):
    copies = [
        pltpu.make_async_copy(source, target, sems.at[at])
        for at, (source, target) in enumerate(
            (
                (signal_in, signal),
                (order_in, order),
                (factors_in.at[pl.ds(0, LOCAL_LEVELS)], factors),
            )
        )
    ]
    for copy in copies:
        copy.start()
    step = freq[...] * lax.broadcasted_iota(jnp.int32, freq.shape, 0)
    cos_column = cosine(step)[:, :1]
    sin_column = -cosine(step + 6)[:, :1]
    shots = signal.shape[0]
    copies[0].wait()

    @pl.loop(0, shots // SAMPLES)
    def _(part):
        start = pl.multiple_of(part * SAMPLES, SAMPLES)
        for sign, column in ((0, cos_column), (1, sin_column)):
            sums = [
                jnp.sum(signal[start + at] * column, axis=0, keepdims=True)
                for at in range(SAMPLES)
            ]
            spectrum[pl.ds(sign * shots + start, SAMPLES), :] = jnp.concatenate(sums, axis=0)

    copies[1].wait()
    parts = split(spectrum[...])
    elements = parts.shape[1]
    element = lax.broadcasted_iota(jnp.int32, (elements, RANK), 0)

    @pl.loop(0, BOXES)
    def _(box):
        place = order[:, pl.ds(pl.multiple_of(box * RANK, RANK), RANK)]
        chosen = jnp.where(element == place, F32(1.0), F32(0.0)).astype(BF16)
        placed = joined(dot(parts, chosen))
        rows = pl.ds(pl.multiple_of(box * shots, shots), shots)
        coeffs[0, rows, :] = placed[:shots]
        coeffs[1, rows, :] = placed[shots:]

    copies[2].wait()
    put(out, local_forward(paired(coeffs), factors))


def core_kernel(own, other, factors, *outs):
    level = LOCAL_LEVELS
    size = outs[0].shape[1] // BOXES
    shots = size * len(outs)
    coeffs = joined(dot(split(paired(own)), factor(factors, level, 0))) + joined(
        dot(split(paired(other)), factor(factors, level, 1))
    )
    for group, out in enumerate(outs):
        starts = [box * shots + group * size for box in range(BOXES)]
        put(out, jnp.concatenate([coeffs[at : at + size] for at in starts], axis=0))


def two_levels(own, near, far, both, factors, far_factors, level):
    first = joined(dot(split(paired(own)), factor(factors, level, 0))) + joined(
        dot(split(paired(near)), factor(factors, level, 1))
    )
    second = joined(dot(split(paired(far)), far_factor(far_factors, 0))) + joined(
        dot(split(paired(both)), far_factor(far_factors, 1))
    )
    return joined(dot(split(first), factor(factors, level + 1, 0))) + joined(
        dot(split(second), factor(factors, level + 1, 1))
    )


def two_adjoints(coeffs, factors, far_factors, level, own, near, far, both):
    parts = split(coeffs)
    first = split(joined(dot_t(parts, factor(factors, level + 1, 0))))
    second = split(joined(dot_t(parts, factor(factors, level + 1, 1))))
    put(own, joined(dot_t(first, factor(factors, level, 0))))
    put(near, joined(dot_t(first, factor(factors, level, 1))))
    put(far, joined(dot_t(second, far_factor(far_factors, 0))))
    put(both, joined(dot_t(second, far_factor(far_factors, 1))))


def forward_kernel(own, near, far, both, factors, far_factors, out, *, level):
    put(out, two_levels(own, near, far, both, factors, far_factors, level))


def adjoint_kernel(a, b, c, d, factors, far_factors, own, near, far, both, *, level):
    coeffs = (paired(a) + paired(b)) + (paired(c) + paired(d))
    two_adjoints(coeffs, factors, far_factors, level, own, near, far, both)


def core_adjoint_kernel(*refs):
    *terms, factors, own, other = refs
    level = LOCAL_LEVELS
    sums = []
    for at in range(0, len(terms), 4):
        a, b, c, d = (paired(ref) for ref in terms[at : at + 4])
        sums.append((a + b) + (c + d))
    size = sums[0].shape[0] // BOXES
    rows = [part[box * size : (box + 1) * size] for box in range(BOXES) for part in sums]
    parts = split(jnp.concatenate(rows, axis=0))
    put(own, joined(dot_t(parts, factor(factors, level, 0))))
    put(other, joined(dot_t(parts, factor(factors, level, 1))))


def local_adjoint_kernel(own, other, factors, freq, out):
    coeffs = paired(own) + paired(other)
    for level in reversed(range(LOCAL_LEVELS)):
        parts = split(coeffs)
        cross = joined(dot_t(parts, factor(factors, level, 1)))
        coeffs = joined(dot_t(parts, factor(factors, level, 0))) + flip_boxes(cross, level)
    rows = coeffs.shape[0]
    out[:rows, :] = coeffs[:, :RANK]
    out[rows : 2 * rows, :] = coeffs[:, RANK:]
    out[2 * rows :, :] = freq[...].astype(F32)


def image_kernel(
    own0, near0, far0, both0, factors, far_factors, weights, reflect, coupling,
    own, near, far, both,
    coeffs, stacked, echo, total,
    *, level, shots,
):
    entered = two_levels(own0, near0, far0, both0, factors, far_factors, level)
    put(coeffs, entered)
    lanes = 2 * RANK

    @pl.loop(0, shots)
    def _(shot):
        real = coeffs[0, pl.ds(shot, BOXES, stride=shots), :]
        imag = coeffs[1, pl.ds(shot, BOXES, stride=shots), :]
        rows = jnp.concatenate([real, imag], axis=1)
        turned = jnp.concatenate([-imag, real], axis=1)
        at = pl.ds(pl.multiple_of(shot * lanes, lanes), lanes)
        stacked[:, at] = jnp.concatenate([rows, turned], axis=0).astype(BF16)

    total[...] = jnp.zeros_like(total)
    couple = block_form(coupling[0], coupling[1])
    block = Q_BLOCK

    @pl.loop(0, weights.shape[1] // block)
    def _(turn):
        start = pl.multiple_of(turn * block, block)
        weight = weights[:, pl.ds(start, block)]
        weight_t = weight.astype(F32).T.astype(BF16)
        rho = reflect[pl.ds(start, block), :].astype(F32)
        rho = jnp.concatenate([rho, rho], axis=1)
        for shot in range(shots):
            at = slice(shot * lanes, (shot + 1) * lanes)
            field = dot(weight_t, stacked[:, at])
            coupled = dot((rho * field).astype(BF16), couple)
            echo[:, at] = (rho * (field + coupled)).astype(BF16)
        total[...] += dot(weight, echo[...])

    @pl.loop(0, shots)
    def _(shot):
        at = pl.ds(pl.multiple_of(shot * lanes, lanes), lanes)
        real, imag = total[:BOXES, at], total[BOXES:, at]
        rows = pl.ds(shot, BOXES, stride=shots)
        coeffs[0, rows, :] = real[:, :RANK] + imag[:, RANK:]
        coeffs[1, rows, :] = real[:, RANK:] - imag[:, :RANK]

    two_adjoints(paired(coeffs), factors, far_factors, level, own, near, far, both)


def time_samples(real, imag):
    (r1, r2, r3), (i1, i2, i3) = real, imag
    half = F32(math.sqrt(0.5))
    r13, r_13, i13, i_13 = r1 + r3, r1 - r3, i1 + i3, i1 - i3
    odd = half * (r_13 - i13)
    even = half * (r_13 + i13)
    return (
        r2 + r13, odd - i2, -r2 - i_13, i2 - even,
        r2 - r13, -odd - i2, i_13 - r2, even + i2,
    )


def summed_kernel(s0, s1, s2, s3, out, energy, *, shots, last):
    spectra = (s0, s1, s2, s3)
    count = shots * BOXES
    freqs = [
        jnp.broadcast_to(spectrum[2 * count : 2 * count + 1, :], (shots, RANK))
        for spectrum in spectra
    ]
    chosen = [
        [jnp.where(jnp.abs(freq - k) < 0.5, F32(1.0), F32(0.0)) for freq in freqs]
        for k in (1, 2, 3)
    ]

    def one_box(box, power):
        rows = pl.ds(pl.multiple_of(box * shots, shots), shots)
        sums = []
        for part in range(2):
            start = pl.multiple_of(part * count + box * shots, shots)
            values = [spectrum[pl.ds(start, shots), :] for spectrum in spectra]
            for weights in chosen:
                terms = [weight * value for weight, value in zip(weights, values)]
                sums.append((terms[0] + terms[1]) + (terms[2] + terms[3]))
        for value in sums:
            power = power + value * value
        for time, value in enumerate(time_samples(sums[:3], sums[3:])):
            if last:
                out[box, pl.ds(time, shots, stride=SAMPLES), :] = value
            else:
                out[time, rows, :] = value
        return power

    power = lax.fori_loop(0, BOXES, one_box, jnp.zeros((shots, RANK), F32))
    column = jnp.sum(power, axis=1, keepdims=True) * (SAMPLES / 2)
    at_shot = lax.broadcasted_iota(jnp.int32, (shots, RANK), 0)
    at_lane = lax.broadcasted_iota(jnp.int32, (shots, RANK), 1)
    row = jnp.sum(jnp.where(at_shot == at_lane, column, F32(0.0)), axis=0, keepdims=True)
    energy[...] = jnp.broadcast_to(row, energy.shape)


def amplitude(energy, clip_level, shots):
    row = jnp.sum(energy[...], axis=0, keepdims=True)
    root_mean = jnp.sqrt(row / (SAMPLES * ELEMENTS) + 1e-6)[:, :shots]
    row = (4.0 + clip_level[...].astype(F32)) / 10.0 * root_mean
    at_shot = lax.broadcasted_iota(jnp.int32, (shots, shots), 0)
    at_lane = lax.broadcasted_iota(jnp.int32, (shots, shots), 1)
    return jnp.sum(jnp.where(at_shot == at_lane, row, F32(0.0)), axis=1, keepdims=True)


def next_kernel(summed, energy, clip_level, freq, factors, out, coeffs, *, shots):
    step = jnp.broadcast_to(freq[:1, :], (shots, RANK))
    cos_values = [cosine(step * time) for time in range(SAMPLES)]
    sin_values = [cosine(step * time + 6) for time in range(SAMPLES)]
    amp = jnp.broadcast_to(amplitude(energy, clip_level, shots), (shots, RANK))
    inverse = 1.0 / amp

    @pl.loop(0, BOXES)
    def _(box):
        rows = pl.ds(pl.multiple_of(box * shots, shots), shots)
        real = jnp.zeros((shots, RANK), F32)
        imag = jnp.zeros((shots, RANK), F32)
        for time in range(SAMPLES):
            value = jnp.clip(summed[time, rows, :], -amp, amp)
            real = real + value * cos_values[time]
            imag = imag - value * sin_values[time]
        coeffs[0, rows, :] = real * inverse
        coeffs[1, rows, :] = imag * inverse

    put(out, local_forward(paired(coeffs), factors))


def order_kernel(summed, order, out):
    parts = split(jnp.concatenate([summed[box] for box in range(BOXES)], axis=1))
    elements = parts.shape[1]
    element = lax.broadcasted_iota(jnp.int32, (RANK, elements), 0)

    @pl.loop(0, elements // (RANK))
    def _(tile):
        start = pl.multiple_of(tile * RANK, RANK)
        chosen = jnp.where(order[...] == element + start, F32(1.0), F32(0.0))
        out[:, pl.ds(start, RANK)] = joined(dot_t(parts, chosen.astype(BF16)))


def clip_kernel(summed, energy, clip_level, out, *, shots):
    amp = amplitude(energy, clip_level, shots)
    for shot in range(shots):
        limit = jnp.broadcast_to(amp[shot : shot + 1, :], (SAMPLES, 1))
        value = summed[shot * SAMPLES : (shot + 1) * SAMPLES, :]
        out[shot] = jnp.clip(value, -limit, limit) / limit


def call(body, outs, operands, raw=0, scratch=(), limit=24, flops=0, **settings):
    def kernel(*refs):
        body(*refs, **settings)

    return pl.pallas_call(
        kernel,
        out_shape=outs,
        in_specs=[RAW if at < raw else VMEM for at in range(len(operands))],
        out_specs=jax.tree.map(lambda _: VMEM, outs),
        scratch_shapes=list(scratch),
        compiler_params=pltpu.CompilerParams(vmem_limit_bytes=limit << 20),
        cost_estimate=pl.CostEstimate(flops=flops, transcendentals=0, bytes_accessed=1 << 20),
    )(*operands)


def exchange(values, axis):
    received = []
    for step, value in enumerate(values, 1):
        pairs = [(source, source ^ step) for source in range(lax.axis_size(axis))]
        received.append(lax.ppermute(value, axis, pairs))
    return received


def on_device(
    excitation,
    freq_index,
    elem_order,
    level_factors,
    image_weights,
    coupling,
    reflectivity,
    clip_level,
):
    shots = excitation.shape[0] // GROUPS
    rows = shots * BOXES
    leaves = lax.axis_size(LEAF)
    factors = level_factors[0, 0]
    weights = image_weights[0].reshape(2 * BOXES, image_weights.shape[3])
    couple = coupling[0]
    clips = clip_level.reshape(1, shots * GROUPS)
    coeff = jax.ShapeDtypeStruct((2, rows, RANK), F32)
    freq = jnp.broadcast_to(freq_index, (SAMPLES, RANK))
    every = shots * GROUPS
    whole = jax.ShapeDtypeStruct((2, every * BOXES, RANK), F32)
    rough = pltpu.VMEM((2, every * BOXES, RANK), F32)


    def far_level(level, axis):
        pairs = [(source, source ^ 2) for source in range(lax.axis_size(axis))]
        return lax.ppermute(factors[level].astype(F32), axis, pairs)

    far_z = far_level(5, "leaf_1")
    far_x = far_level(7, "leaf_0")
    coeffs = call(
        first_kernel,
        whole,
        (excitation, elem_order, factors, freq),
        raw=3,
        scratch=[
            pltpu.VMEM(excitation.shape, F32),
            pltpu.VMEM(elem_order.shape, jnp.int32),
            pltpu.VMEM((LOCAL_LEVELS, *factors.shape[1:]), BF16),
            pltpu.VMEM((2 * every, excitation.shape[2]), F32),
            rough,
            pltpu.SemaphoreType.DMA((3,)),
        ],
        flops=8_000_000_000,
        limit=53,
    )

    def levels_up(coeffs):
        received = exchange([coeffs] * 3, "leaf_1")
        coeffs = call(
            forward_kernel, coeff, (coeffs, *received, factors, far_z), flops=1_000_000_000, level=5
        )
        received = exchange([coeffs] * 3, "leaf_0")
        return call(
            image_kernel,
            (coeff,) * 4,
            (coeffs, *received, factors, far_x, weights, reflectivity, couple),
            scratch=[
                pltpu.VMEM((2, rows, RANK), F32),
                pltpu.VMEM((2 * BOXES, shots * 2 * RANK), BF16),
                pltpu.VMEM((Q_BLOCK, shots * 2 * RANK), BF16),
                pltpu.VMEM((2 * BOXES, shots * 2 * RANK), F32),
            ],
            limit=36,
            flops=8_000_000_000,
            level=7,
            shots=shots,
        )

    def levels_down(own, *sent):
        own, *sent = call(
            adjoint_kernel,
            (coeff,) * 4,
            (own, *exchange(sent, "leaf_0"), factors, far_z),
            flops=1_000_000_000,
            level=5,
        )
        return own, *exchange(sent, "leaf_1")

    for iteration in range(ITERS):
        last = iteration == ITERS - 1
        (other,) = exchange([coeffs], "leaf_2")
        started = call(
            core_kernel, (coeff,) * GROUPS, (coeffs, other, factors), flops=1_000_000_000
        )
        terms = []
        for coeffs in started:
            terms += levels_down(*levels_up(coeffs))
        own, sent = call(core_adjoint_kernel, (whole,) * 2, (*terms, factors), flops=1_000_000_000)
        (other,) = exchange([sent], "leaf_2")
        spectrum = call(
            local_adjoint_kernel,
            jax.ShapeDtypeStruct((2 * every * BOXES + SAMPLES, RANK), F32),
            (own, other, factors, freq),
            flops=2_000_000_000,
        )
        shape = (BOXES, every * SAMPLES, RANK) if last else (SAMPLES, every * BOXES, RANK)
        summed, energy = call(
            summed_kernel,
            (jax.ShapeDtypeStruct(shape, F32), jax.ShapeDtypeStruct((leaves, RANK), F32)),
            (spectrum, *exchange([spectrum] * 3, "band")),
            flops=1_000_000_000,
            shots=every,
            last=last,
        )
        energy = lax.all_to_all(energy, LEAF, 0, 0, tiled=True)
        if not last:
            coeffs = call(
                next_kernel,
                whole,
                (summed, energy, clips, freq, factors),
                scratch=[rough],
                flops=2_000_000_000,
                shots=every,
            )
    ordered = call(
        order_kernel,
        jax.ShapeDtypeStruct((every * SAMPLES, excitation.shape[2]), F32),
        (summed, elem_order),
        flops=4_000_000_000,
    )
    return call(
        clip_kernel,
        jax.ShapeDtypeStruct(excitation.shape, F32),
        (ordered, energy, clips),
        flops=500_000_000,
        shots=every,
    )


def solution(mesh):
    finer = Mesh(
        mesh.devices.reshape(4, 4, 2, mesh.shape["band"]), ("leaf_0", "leaf_1", "leaf_2", "band")
    )
    placed = (
        P(None, None, LEAF),
        P("band"),
        P(LEAF, None),
        P("band", LEAF, None, None, None, None, None),
        P("band", None, None, LEAF),
        P("band", None, None, None),
        P(LEAF, None),
        P(),
    )

    return jax.shard_map(
        on_device, mesh=finer, in_specs=placed, out_specs=P(None, None, LEAF), check_vma=False
    )
```
